32 devices in a mesh: grp: 4 (over y, x), dom: 8 (over z, core).
Axes of the slice: x: 2, y: 2, z: 4, core: 2. Of those that a mesh axis runs over, the one named last changes fastest.
Arguments:
- fields: float32 [210, 32768], P(None, ('grp', 'dom')), may hold values from -6 to 6
- metric: float32 [9, 32768], P(None, ('grp', 'dom')), may hold values from -5 to 5
- normals: float32 [12, 32768], P(None, ('grp', 'dom')), may hold values from -3 to 3
- fscale: float32 [4, 32768], P(None, ('grp', 'dom')), may hold values from 0.5 to 4
- orders: int32 [32768], P(('grp', 'dom')), may hold values from 1 to 4, as said below
- slots: int32 [32768], P(('grp', 'dom')), may hold values from 0 to 511, as said below
- send_faces: int32 [294912], P(('grp', 'dom')), may hold values from 0 to 8192, as said below
- recv_faces: int32 [262144], P(('grp', 'dom')), may hold values from 0 to 9216, as said below
- dmat: float32 [4, 105, 35], P('grp'), may hold values from -4 to 4
- tmat: float32 [4, 60, 35], P('grp'), may hold values from -4 to 4
- lmat: float32 [4, 35, 60], P('grp'), may hold values from -3 to 3
Outputs:
- rhs: float32 [210, 65536], P(None, ('grp', 'dom'))
The draws below stay inside these ranges and needn't reach their ends.
Inputs may be any that keep to these rules, and one draw needn't show every extreme that they name: `orders`: on each device every order from 1 to 4 is held by at least one element and by at most 512; one order is held by exactly 512. The elements of one device that share an order have distinct slots. `send_faces`: each entry names a face of an occupied slot of the sending bucket or equals 4 * 2048 (nothing); in each list the items in use stand first. `recv_faces`: every face of an occupied slot names a distinct received item that is in use, and every item in use is named by exactly one face; faces of empty slots hold 9216. A list carries at most 768 items in use, and some list carries exactly 768.
All inputs are finite; a program needn't handle non-finite values.
Results may differ from the reference program's by a relative error of at most 0.0003.
Values sent between devices are 32-bit elements; how exact they have to be, the bound alone decides.
A program may use at most 128 MiB of HBM per device.

```python
import math
import jax
import jax.numpy as jnp
from jax import lax

NPM = 35
FPTS = 15
ORDERS = 4
E_DEV = 1024
CAP = 512
NB = 2048
FCAP = 768
LISTS = 9216
DOMS = 8
ELEMS = 32768
SLOTS = 65536
DEVICES = 32


def mesh_tables(key):
    base = jax.random.fold_in(key, 4242)
    streams = jax.random.split(base, 7)
    spare = E_DEV - CAP
    leading = jax.random.randint(streams[0], (DEVICES,), 0, ORDERS)
    cuts = jax.random.randint(streams[1], (DEVICES, 2), 0, spare - 2)
    lower = jnp.minimum(cuts[:, 0], cuts[:, 1]) + 1
    upper = jnp.maximum(cuts[:, 0], cuts[:, 1]) + 2
    rank_sizes = jnp.stack([jnp.full((DEVICES,), CAP, jnp.int32), lower, upper - lower, spare - upper], 1)
    rank_ends = jnp.cumsum(rank_sizes, 1)
    rank_starts = rank_ends - rank_sizes
    position = jax.vmap(lambda sub_key: jax.random.permutation(sub_key, E_DEV))(jax.random.split(streams[2], DEVICES)).astype(jnp.int32)
    rank_of = jnp.sum((position[:, :, None] >= rank_ends[:, None, :]).astype(jnp.int32), 2)
    within = position - jnp.take_along_axis(rank_starts, rank_of, 1)
    order_index = (leading[:, None] + rank_of) % ORDERS
    shuffles = jax.vmap(lambda sub_key: jax.random.permutation(sub_key, CAP))(jax.random.split(streams[3], DEVICES * ORDERS)).astype(jnp.int32)
    shuffles = shuffles.reshape(DEVICES, ORDERS * CAP)
    slot_value = jnp.take_along_axis(shuffles, order_index * CAP + within, 1)
    device_ids = jnp.arange(DEVICES, dtype=jnp.int32)[:, None]
    bucket_dev = order_index * DOMS + device_ids % DOMS
    bucket_col = device_ids // DOMS * CAP + slot_value
    occupied = jnp.zeros((DEVICES, NB), jnp.int32).at[bucket_dev, bucket_col].set(1)
    face_total = 4 * jnp.sum(occupied, 1)
    occupied_slots = jnp.argsort((1 - occupied) * NB + jnp.arange(NB, dtype=jnp.int32)[None], axis=1).astype(jnp.int32)
    enumerated = jnp.arange(4 * NB, dtype=jnp.int32)
    face_of = (enumerated % 4)[None] * NB + occupied_slots[:, enumerated // 4]
    valid = enumerated[None] < face_total[:, None]
    list_total = 3 * ORDERS
    first_list = jax.random.randint(streams[4], (DEVICES,), 0, list_total)
    leading_count = jnp.minimum(face_total, FCAP)
    remainder = face_total - leading_count
    share = remainder // (list_total - 1)
    extra = remainder % (list_total - 1)
    offset = (jnp.arange(list_total, dtype=jnp.int32)[None] - first_list[:, None]) % list_total
    counts = jnp.where(offset == 0, leading_count[:, None], share[:, None] + (offset - 1 < extra[:, None]).astype(jnp.int32))
    list_ends = jnp.cumsum(counts, 1)
    list_starts = list_ends - counts
    face_shuffle = jax.vmap(lambda sub_key: jax.random.permutation(sub_key, 4 * NB))(jax.random.split(streams[5], DEVICES)).astype(jnp.int32)
    scores = jnp.where(valid, face_shuffle, 4 * NB + enumerated[None])
    ranking = jnp.argsort(jnp.argsort(scores, axis=1), axis=1).astype(jnp.int32)
    list_of = jnp.sum((ranking[:, :, None] >= list_ends[:, None, :]).astype(jnp.int32), 2)
    list_of = jnp.minimum(list_of, list_total - 1)
    place_in = ranking - jnp.take_along_axis(list_starts, list_of, 1)
    entry_value = jnp.where(valid, list_of * FCAP + place_in, LISTS)
    targets = jnp.where(valid, face_of, 4 * NB)
    receive = jnp.full((DEVICES, 4 * NB + 1), LISTS, jnp.int32).at[device_ids, targets].set(entry_value)[:, :4 * NB]
    sender_ids = jnp.arange(DEVICES, dtype=jnp.int32)[:, None, None]
    direction = jnp.arange(3, dtype=jnp.int32)[None, :, None]
    peer_group = jnp.arange(ORDERS, dtype=jnp.int32)[None, None, :]
    receiver = peer_group * DOMS + (sender_ids % DOMS + direction - 1) % DOMS
    list_index = direction * ORDERS + sender_ids // DOMS
    wanted = counts[receiver, list_index]
    picks = jax.random.randint(streams[6], (DEVICES, 3, ORDERS, FCAP), 0, 2 ** 30) % face_total[:, None, None, None]
    chosen = jnp.take_along_axis(face_of, picks.reshape(DEVICES, -1), 1).reshape(DEVICES, 3, ORDERS, FCAP)
    sending = jnp.where(jnp.arange(FCAP, dtype=jnp.int32)[None, None, None] < wanted[..., None], chosen, 4 * NB)
    return ((order_index + 1).reshape(ELEMS), slot_value.reshape(ELEMS), sending.reshape(DEVICES * LISTS), receive.reshape(DEVICES * 4 * NB))


def draw_orders(key, part):
    return mesh_tables(key)[0]


def draw_slots(key, part):
    return mesh_tables(key)[1]


def draw_send_faces(key, part):
    return mesh_tables(key)[2]


def draw_recv_faces(key, part):
    return mesh_tables(key)[3]


def block_levels(rng, extent, shards, least, largest):
    factor_of = 1.0
    for dim, shards_of in shards:
        draws = jax.random.uniform(jax.random.fold_in(jax.random.fold_in(rng, 6), dim), (shards_of,), jnp.float32, least / len(shards), largest / len(shards))
        factor_of = factor_of * jnp.repeat(jnp.exp(draws), extent[dim] // shards_of).reshape((-1,) + (1,) * (len(extent) - 1 - dim))
    return factor_of


def bell_draw(rng, shape, deviation, bound, cuts=(), kind=jnp.bfloat16):
    level = block_levels(rng, shape, cuts, -0.22, 0.18) if cuts else 1.0
    values = jax.random.normal(rng, shape, jnp.float32) * deviation * level
    return jnp.minimum(jnp.maximum(values, -bound), bound).astype(kind)


def setup_inputs(seed: int = 0) -> dict:
    key_list = jax.random.split(jax.random.key(seed), 12)
    return {
        "fields": bell_draw(key_list[0], (6 * NPM, ELEMS), 1.0, 6.0, ((1, 32),), jnp.float32),
        "metric": bell_draw(key_list[1], (9, ELEMS), 1.0, 5.0, ((1, 32),), jnp.float32),
        "normals": bell_draw(key_list[2], (12, ELEMS), 0.6, 3.0, ((1, 32),), jnp.float32),
        "fscale": jnp.clip(jnp.exp(math.log(4.0) - 2.0794415 * jax.random.uniform(key_list[3], (4, ELEMS), jnp.float32) ** block_levels(key_list[3], (4, ELEMS), ((1, 32),), -0.2, 0.2)), 0.5, 4.0),
        "orders": draw_orders(jax.random.fold_in(key_list[11], 71), 0),
        "slots": draw_slots(jax.random.fold_in(key_list[11], 71), 0),
        "send_faces": draw_send_faces(jax.random.fold_in(key_list[11], 71), 0),
        "recv_faces": draw_recv_faces(jax.random.fold_in(key_list[11], 71), 0),
        "dmat": bell_draw(key_list[8], (ORDERS, 3 * NPM, NPM), 0.3, 4.0, ((0, 4),), jnp.float32),
        "tmat": bell_draw(key_list[9], (ORDERS, 4 * FPTS, NPM), 0.3, 4.0, ((0, 4),), jnp.float32),
        "lmat": bell_draw(key_list[10], (ORDERS, NPM, 4 * FPTS), 0.2, 3.0, ((0, 4),), jnp.float32),
    }


exact_prec = lax.Precision.HIGHEST


def order_mask(order_index):
    node_total = (order_index + 2) * (order_index + 3) * (order_index + 4) // 6
    return (jnp.arange(NPM, dtype=jnp.int32) < node_total).astype(jnp.float32)


def cross_of(first_vec, second_vec):
    return [first_vec[1] * second_vec[2] - first_vec[2] * second_vec[1],
            first_vec[2] * second_vec[0] - first_vec[0] * second_vec[2],
            first_vec[0] * second_vec[1] - first_vec[1] * second_vec[0]]


def volume_terms(coefficients, metric_cols, deriv_mats):
    derived = jnp.einsum('anm,qms->qans', deriv_mats, coefficients, precision=exact_prec)

    def partial_of(component, direction):
        return (metric_cols[0, direction][None] * derived[component, 0]
                + metric_cols[1, direction][None] * derived[component, 1]
                + metric_cols[2, direction][None] * derived[component, 2])

    curl_h = [partial_of(5, 1) - partial_of(4, 2), partial_of(3, 2) - partial_of(5, 0), partial_of(4, 0) - partial_of(3, 1)]
    curl_e = [partial_of(2, 1) - partial_of(1, 2), partial_of(0, 2) - partial_of(2, 0), partial_of(1, 0) - partial_of(0, 1)]
    return jnp.stack(curl_h + [-value for value in curl_e], 0)


def face_flux(own_traces, neighbour, normal_cols, scale_cols):
    own_split = own_traces.reshape(6, FPTS, -1)
    far_split = neighbour.reshape(6, FPTS, -1)
    jump_e = [far_split[c] - own_split[c] for c in range(3)]
    jump_h = [far_split[c + 3] - own_split[c + 3] for c in range(3)]
    normal = [normal_cols[c] for c in range(3)]
    normal_e = normal[0] * jump_e[0] + normal[1] * jump_e[1] + normal[2] * jump_e[2]
    normal_h = normal[0] * jump_h[0] + normal[1] * jump_h[1] + normal[2] * jump_h[2]
    turn_h = cross_of(normal, jump_h)
    turn_e = cross_of(normal, jump_e)
    flux_e = [0.5 * scale_cols * (turn_h[c] + jump_e[c] - normal[c] * normal_e) for c in range(3)]
    flux_h = [0.5 * scale_cols * (-turn_e[c] + jump_h[c] - normal[c] * normal_h) for c in range(3)]
    return jnp.stack(flux_e + flux_h, 0)


def block_rhs(bucket, own_traces, neighbour, deriv_mats, lift_mat):
    slot_count = bucket.shape[1]
    coefficients = bucket[:6 * NPM].reshape(6, NPM, slot_count)
    metric_cols = bucket[6 * NPM:6 * NPM + 9].reshape(3, 3, slot_count)
    normal_cols = bucket[6 * NPM + 9:6 * NPM + 21].reshape(3, 1, 4 * slot_count)
    scale_cols = bucket[6 * NPM + 21:6 * NPM + 25].reshape(1, 4 * slot_count)
    volume = volume_terms(coefficients, metric_cols, deriv_mats)
    flux = face_flux(own_traces, neighbour, normal_cols, scale_cols).reshape(6, FPTS * 4, slot_count)
    lifted = jnp.einsum('mp,qps->qms', lift_mat, flux, precision=exact_prec)
    return (volume + lifted).reshape(6 * NPM, slot_count)


def reference(fields, metric, normals, fscale, orders, slots, send_faces, recv_faces, dmat, tmat, lmat):
    element_total = fields.shape[1]
    positions = jnp.arange(element_total, dtype=jnp.int32)
    owner = positions // E_DEV
    column = ((orders - 1) * DOMS + owner % DOMS) * NB + (owner // DOMS) * CAP + slots
    inverse = jnp.full((SLOTS,), element_total, jnp.int32).at[column].set(positions)
    payload = jnp.concatenate([fields, metric, normals, fscale], 0)
    padded = jnp.concatenate([payload, jnp.zeros((payload.shape[0], 1), jnp.float32)], 1)

    def gather_block(block_id):
        picked = lax.dynamic_slice_in_dim(inverse, block_id * NB, NB)
        return jnp.take(padded, picked, axis=1)

    def matrices(block_id):
        order_index = block_id // DOMS
        node_mask = order_mask(order_index)
        deriv_mats = dmat[order_index].reshape(3, NPM, NPM) * node_mask[None, :, None] * node_mask[None, None, :]
        trace_mat = tmat[order_index] * node_mask[None, :]
        lift_mat = lmat[order_index] * node_mask[:, None]
        return deriv_mats, trace_mat, lift_mat

    def traces_of(block_id):
        bucket = gather_block(block_id)
        trace_mat = matrices(block_id)[1]
        coefficients = bucket[:6 * NPM].reshape(6, NPM, NB)
        traced = jnp.einsum('pm,qms->qps', trace_mat, coefficients, precision=exact_prec)
        return traced.reshape(6 * FPTS, 4 * NB)

    traces = lax.map(traces_of, jnp.arange(DEVICES, dtype=jnp.int32))
    entries = jnp.arange(LISTS, dtype=jnp.int32)
    direction = entries // (ORDERS * FCAP)
    peer_group = (entries // FCAP) % ORDERS
    places = entries % FCAP
    receiver = jnp.arange(DEVICES, dtype=jnp.int32)[:, None]
    sender = peer_group[None] * DOMS + (receiver % DOMS - direction[None] + 1) % DOMS
    position = (direction[None] * ORDERS + receiver // DOMS) * FCAP + places[None]
    send_table = send_faces.reshape(DEVICES, LISTS)
    sent_face = send_table[sender, position]
    missing = DEVICES * 4 * NB
    flat_id = jnp.where(sent_face < 4 * NB, sender * (4 * NB) + sent_face, missing)
    recv_table = recv_faces.reshape(DEVICES, 4 * NB)

    def rhs_of(block_id):
        bucket = gather_block(block_id)
        deriv_mats, trace_mat, lift_mat = matrices(block_id)
        entry_ids = recv_table[block_id]
        global_ids = flat_id[block_id][jnp.minimum(entry_ids, LISTS - 1)]
        global_ids = jnp.where(entry_ids < LISTS, global_ids, missing)
        valid = (global_ids < missing).astype(jnp.float32)
        src_block = jnp.minimum(global_ids // (4 * NB), DEVICES - 1)
        face_ids = global_ids % (4 * NB)
        neighbour = traces[src_block, :, face_ids].T * valid[None]
        return block_rhs(bucket, traces[block_id], neighbour, deriv_mats, lift_mat)

    blocks = lax.map(rhs_of, jnp.arange(DEVICES, dtype=jnp.int32))
    return jnp.transpose(blocks, (1, 0, 2)).reshape(6 * NPM, SLOTS)
```

```python
import functools

import jax
import jax.numpy as jnp
from jax import lax
from jax.experimental import pallas as pl
from jax.experimental.pallas import tpu as pltpu
from jax.sharding import PartitionSpec as P

NPM = 35
FPTS = 15
COMPS = 6
FACES = 4
PP = 16
DP = 40
LANES = 128
TR = COMPS * PP
NODES = (4, 10, 20, 35)
STARTS = (0, 4, 10, 20)
N1 = NODES[0]
LOW = COMPS * N1
CODED = 32
METRIC, NORMAL, SCALE, ONE, GEO = 0, 9, 21, 25, 26
GROWS = 32
ROWS = 240
SENT = tuple(-(-(GEO + COMPS * n) // 8) * 8 for n in NODES)
BASES = tuple(GEO + COMPS * s for s in STARTS)
RELAYED = (2, 0)
MESH = pl.DeviceIdType.MESH
F32 = jnp.float32
BF16 = jnp.bfloat16
EXACT = lax.Precision.HIGHEST


def split(x):
    high = x.astype(BF16)
    low = (x - high.astype(F32)).astype(BF16)
    return high, low


def dot3(a, b, dims):
    ah, al = a
    bh, bl = b

    def mul(x, y):
        return lax.dot_general(x, y, (dims, ((), ())), preferred_element_type=F32)

    return mul(ah, bh) + (mul(ah, bl) + mul(al, bh))


def exact_dot(a, b, dims=((1,), (0,))):
    return lax.dot_general(a, b, (dims, ((), ())), precision=EXACT, preferred_element_type=F32)


def iotas(shape):
    return lax.broadcasted_iota(jnp.int32, shape, 0), lax.broadcasted_iota(jnp.int32, shape, 1)


def ones_where(cond):
    return jnp.where(cond, 1.0, 0.0).astype(F32)


VM = pl.BlockSpec(memory_space=pltpu.VMEM)
SM = pl.BlockSpec(memory_space=pltpu.SMEM)


def gather_block(index_ref, base, table, tmp):
    for i in range(LANES):
        tmp[i : i + 1, :] = table[pl.ds(index_ref[base + i], 1), :]


def flat_row(block):
    return jnp.concatenate([block[i : i + 1, :] for i in range(block.shape[0])], axis=1)


CURL = ((5, 1, 4, 2), (3, 2, 5, 0), (4, 0, 3, 1), (1, 2, 2, 1), (2, 0, 0, 2), (0, 1, 1, 0))


def place(c, shape):
    i, r = iotas(shape)
    target = BASES[3] + c * (NODES[3] - STARTS[3]) + (i - STARTS[3])
    for b in (2, 1, 0):
        width = NODES[b] - STARTS[b]
        target = jnp.where(i < NODES[b], BASES[b] + c * width + (i - STARTS[b]), target)
    return i, r, target


def move_kernel(
    groups, doms, cap, list_size,
    send_ref, orders_ref, slots_ref, fields_ref, metric_ref, normals_ref, fscale_ref, recv_ref, dmat_ref, tmat_ref, lmat_ref,
    far_ref, own_ref, vol_ref, geo_ref, lift_ref,
    pay, bsend, bucket, table, low_table, tmp, sbuf, arrived, relay, wide, wcat_h, wcat_l, tr_h, tr_l, dx_h, dx_l,
    derivs, l1x, t1x, faces_out, faces_in,
    bsend_sem, brecv_sem, ssem, rsem, relay_send, relay_recv, l1_send, l1_recv, t1_send, t1_recv, fsend_sem, frecv_sem,
):
    g = lax.axis_index("grp")
    p = lax.axis_index("dom")
    slots = groups * cap
    blocks = list_size // LANES
    elements = 2 * cap
    barrier = pltpu.get_barrier_semaphore()

    def dom_of(j):
        return lax.rem(p + j - 1 + doms, doms)

    for b in range(groups):
        bucket[b, SENT[0] : ROWS, :] = jnp.zeros((ROWS - SENT[0], cap), F32)
    for j in (1, 2, 0):
        for d in range(groups):
            if (j, d) != (1, 0):
                pl.semaphore_signal(
                    barrier, inc=1, device_id=(lax.rem(g + d, groups), dom_of(j)), device_id_type=MESH
                )

    pay[METRIC : METRIC + 9, :] = metric_ref[...]
    pay[NORMAL : NORMAL + 12, :] = normals_ref[...]
    pay[SCALE : SCALE + 4, :] = fscale_ref[...]
    pay[ONE : ONE + 1, :] = jnp.ones((1, elements), F32)
    for b in range(4):
        width = NODES[b] - STARTS[b]
        for c in range(COMPS):
            at = BASES[b] + c * width
            pay[at : at + width, :] = fields_ref[c * NPM + STARTS[b] : c * NPM + NODES[b], :]
    pay[GEO + COMPS * NPM : ROWS, :] = jnp.zeros((ROWS - GEO - COMPS * NPM, elements), F32)
    target = flat_row((orders_ref[...] - 1) * cap + slots_ref[...])
    high, low = split(pay[...])
    both = jnp.concatenate([high, low], axis=0)
    step = min(cap, 256)

    def build(h, dst):
        for k in range(0, cap, step):
            ids = lax.broadcasted_iota(jnp.int32, (step, elements), 0) + (h * cap + k)
            hot = jnp.where(ids == target, 1.0, 0.0).astype(BF16)
            out = lax.dot_general(both, hot, (((1,), (1,)), ((), ())), preferred_element_type=F32)
            dst[:, k : k + step] = out[:ROWS] + out[ROWS:]

    def goal(i):
        top = groups - 1 - i
        return top - jnp.where(top <= g, 1, 0)

    def bucket_copy(i, rows):
        return pltpu.make_async_remote_copy(
            src_ref=bsend.at[i, pl.ds(0, rows)],
            dst_ref=bucket.at[g, pl.ds(0, rows)],
            send_sem=bsend_sem.at[i],
            recv_sem=brecv_sem.at[g],
            device_id=(goal(i), p),
            device_id_type=MESH,
        )

    def for_goal(i, act):
        for h in (groups - 1 - i, groups - 2 - i):
            @pl.when(goal(i) == h)
            def _(h=h):
                act(bucket_copy(i, SENT[h]))

    build(goal(0), bsend.at[0])
    pl.semaphore_wait(barrier, 3 * groups - 1)
    for i in range(1, groups - 1):
        build(goal(i), bsend.at[i])
        for_goal(i - 1, lambda copy: copy.start())
    build(g, bucket.at[g])
    for_goal(groups - 2, lambda copy: copy.start())

    own_nodes = (g + 2) * (g + 3) * (g + 4) // 6
    wide[...] = jnp.zeros_like(wide)
    wide[0, 0 : FPTS * FACES, 0:NPM] = tmat_ref[...]
    wide[1, 0:NPM, 0 : FPTS * FACES] = lmat_ref[...]
    for a in range(3):
        wide[2 + a, 0:NPM, 0:NPM] = dmat_ref[a * NPM : (a + 1) * NPM, :]
    i, r = iotas((FACES * PP, LANES))
    order_points = ones_where((r == (i & (PP - 1)) * FACES + (i // PP)) & ((i & (PP - 1)) < FPTS))
    trace = exact_dot(order_points, wide[0])
    lift = exact_dot(wide[1, 0:DP], order_points, ((1,), (1,)))
    row = lax.broadcasted_iota(jnp.int32, (DP, FACES * PP), 0)
    lift = jnp.where(row < own_nodes, lift, 0.0)
    tr_f = [[] for _ in range(FACES)]
    node = lax.broadcasted_iota(jnp.int32, (DP, ROWS), 0)
    for c in range(COMPS):
        i, r, at = place(c, (LANES, ROWS))
        spread = ones_where((r == at) & (i < own_nodes) & (i < NPM))
        part = exact_dot(trace, spread)
        for f in range(FACES):
            tr_f[f].append(part[f * PP : (f + 1) * PP])
        for a in range(3):
            block = exact_dot(wide[2 + a, 0:DP], spread)
            block = split(jnp.where(node < own_nodes, block, 0.0))
            at_row = (a * COMPS + c) * DP
            dx_h[at_row : at_row + DP, :] = block[0]
            dx_l[at_row : at_row + DP, :] = block[1]
    tr_f = [jnp.concatenate(parts + [jnp.zeros((LANES - TR, ROWS), F32)], 0) for parts in tr_f]

    def fan(f):
        i, r = iotas((FACES * PP, LANES))
        return ones_where(i == f * PP + (r & (PP - 1)))

    def weight_copy(kind, h):
        src, send, recv = ((l1x, l1_send, l1_recv), (t1x, t1_send, t1_recv))[kind]
        return pltpu.make_async_remote_copy(
            src_ref=src, dst_ref=src, send_sem=send.at[h], recv_sem=recv.at[0],
            device_id=(h, p), device_id_type=MESH,
        )

    def face_copy(s, j):
        return pltpu.make_async_remote_copy(
            src_ref=faces_out.at[j * groups + s],
            dst_ref=faces_in.at[j],
            send_sem=fsend_sem.at[j * groups + s],
            recv_sem=frecv_sem.at[j],
            device_id=(s, lax.rem(p - j + 1 + doms, doms)),
            device_id_type=MESH,
        )

    def face_local():
        return pltpu.make_async_copy(faces_out.at[groups], faces_in.at[1], frecv_sem.at[1])

    @pl.when(g == 0)
    def _():
        i, r = iotas((LOW, DP))
        picked = exact_dot(ones_where(r == (i & (N1 - 1))), lift)
        i, r = iotas((CODED, LANES))
        picked_t = exact_dot(ones_where((r == (i & (N1 - 1))) & (i < LOW)), trace, ((1,), (1,)))
        for f in range(FACES):
            i, r = iotas((LOW, LANES))
            l1x[f * LOW : (f + 1) * LOW, :] = jnp.where((r // PP) == (i // N1), exact_dot(picked, fan(f)), 0.0)
            i, r = iotas((CODED, LANES))
            t1x[:, f * LANES : (f + 1) * LANES] = jnp.where(
                (r // PP) == (i // N1), exact_dot(picked_t, fan(f)), 0.0
            )
        rows = slots // LANES
        count = -(-(3 * groups * blocks) // 8) * 8
        found = jnp.zeros((count, LANES), F32)
        for f in range(1, FACES):
            entry = flat_row(recv_ref[f * rows : (f + 1) * rows, :])
            upper, lower = entry // LANES, entry & (LANES - 1)
            a = jnp.where(lax.broadcasted_iota(jnp.int32, (count, slots), 0) == upper, float(f), 0.0).astype(BF16)
            b = jnp.where(lax.broadcasted_iota(jnp.int32, (LANES, slots), 0) == lower, 1.0, 0.0).astype(BF16)
            found = found + lax.dot_general(a, b, (((1,), (1,)), ((), ())), preferred_element_type=F32)
        for n in range(3 * groups):
            faces_out[n, 0:blocks, :] = found[n * blocks : (n + 1) * blocks]
        for kind in range(2):
            for h in range(1, groups):
                weight_copy(kind, h).start()
        for s in range(groups):
            for j in range(3):
                (face_local() if (s, j) == (0, 1) else face_copy(s, j)).start()

    @pl.when(g != 0)
    def _():
        weight_copy(0, 1).wait_recv()

    for f in range(FACES):
        at = f * 2 * LANES
        for k, piece in enumerate(split(tr_f[f])):
            (tr_h, tr_l)[k][f * TR : (f + 1) * TR, :] = piece[:TR]
            (wcat_h, wcat_l)[k][at : at + LANES, :] = piece
        lowered = exact_dot(l1x[...], tr_f[f])
        filled = jnp.concatenate([lowered, jnp.zeros((LANES - TR, ROWS), F32)], 0)
        for k, piece in enumerate(split(filled)):
            (wcat_h, wcat_l)[k][at + LANES : at + 2 * LANES, :] = piece

        @pl.when(g == 0)
        def _(f=f, at=at, lowered=lowered):
            i, r = iotas((LANES, ROWS))
            coded = jnp.where((i < LOW) & (r == GEO + i), 1.0, 0.0) + jnp.where((i == LOW) & (r == ONE), float(f), 0.0)
            wcat_h[at : at + LANES, :] = coded.astype(BF16)
            wcat_l[at : at + LANES, :] = jnp.zeros((LANES, ROWS), BF16)
            i, r = iotas((TR, TR))
            pick = ones_where(((i & (PP - 1)) < N1) & (r == f * LOW + (i // PP) * N1 + (i & (PP - 1))))
            for k, piece in enumerate(split(exact_dot(pick, lowered))):
                (tr_h, tr_l)[k][f * TR : (f + 1) * TR, :] = piece

    i, r = iotas((DP, FACES * PP))
    unit = ones_where((i < N1) & ((r & (PP - 1)) == i))
    lift_ref[...] = jnp.where(g == 0, unit, lift)

    for t in (table, low_table):
        t[FACES * slots : FACES * slots + 8, :] = jnp.zeros((8, LANES), F32)

    def make_tables(b):
        coefs = split(bucket[b].T)
        for f in range(FACES):
            w = tuple(x[f * 2 * LANES : (f + 1) * 2 * LANES, :] for x in (wcat_h, wcat_l))
            rows = dot3(coefs, w, ((1,), (1,)))
            at = pl.multiple_of(f * slots + b * cap, LANES)
            table[pl.ds(at, cap), :] = rows[:, :LANES]
            low_table[pl.ds(at, cap), :] = rows[:, LANES:]

    def arrive(b):
        for h in range(groups):
            @pl.when(g == h)
            def _(h=h):
                pltpu.make_async_remote_copy(
                    src_ref=bsend.at[0, pl.ds(0, SENT[h])],
                    dst_ref=bucket.at[b, pl.ds(0, SENT[h])],
                    send_sem=bsend_sem.at[0],
                    recv_sem=brecv_sem.at[b],
                    device_id=(b, p),
                    device_id_type=MESH,
                ).wait_recv()

    def table_step(k, _):
        b = lax.rem(g + k, groups)

        @pl.when(k > 0)
        def _():
            arrive(b)

        make_tables(b)
        return 0

    lax.fori_loop(0, groups, table_step, 0)

    def list_copy(j, h, rows, dev=None, dst=None, recv=None):
        n = j * groups + h
        return pltpu.make_async_remote_copy(
            src_ref=sbuf.at[n, pl.ds(0, rows)],
            dst_ref=(arrived.at[j * groups + g] if dst is None else dst).at[pl.ds(0, rows)],
            send_sem=ssem.at[n],
            recv_sem=rsem.at[j * groups + g] if recv is None else recv,
            device_id=(h, dom_of(j)) if dev is None else dev,
            device_id_type=MESH,
        )

    def local_copy(h, rows):
        n = groups + h
        return pltpu.make_async_copy(sbuf.at[n, pl.ds(0, rows)], arrived.at[n, pl.ds(0, rows)], rsem.at[n])

    def relay_in(j):
        k = RELAYED.index(j)
        return list_copy(j, 1, TR, dev=(0, dom_of(j)), dst=relay.at[k], recv=relay_recv.at[k])

    def relay_out(j):
        k = RELAYED.index(j)
        return pltpu.make_async_remote_copy(
            src_ref=relay.at[k], dst_ref=arrived.at[j * groups + 2], send_sem=relay_send.at[k],
            recv_sem=rsem.at[j * groups + 2], device_id=(1, p), device_id_type=MESH,
        )

    def for_send(j, h, act, act_local):
        if h == 0:
            if j != 1:
                act(list_copy(j, h, LOW))
            else:
                @pl.when(g != 0)
                def _():
                    act(list_copy(j, h, LOW))

                @pl.when(g == 0)
                def _():
                    act_local(local_copy(h, LOW))
            return

        @pl.when(g == 0)
        def _():
            act(list_copy(j, h, CODED))

        plain = g != 0
        if j == 1:
            plain = jnp.logical_and(plain, g != h)

            @pl.when(g == h)
            def _():
                act_local(local_copy(h, TR))
        if h == 1 and j in RELAYED:
            plain = jnp.logical_and(plain, g != 2)

            @pl.when(g == 2)
            def _():
                act(relay_in(j))

        @pl.when(plain)
        def _():
            act(list_copy(j, h, TR))

    order = [(j, h) for j in (2, 0, 1) for h in (1, 3, 2)] + [(j, 0) for j in (2, 0, 1)]
    before = None
    for j, h in order:
        n = j * groups + h
        if h == 0:
            @pl.when(jnp.logical_or(g != 0, j != 1))
            def _(j=j):
                pltpu.make_async_remote_copy(
                    src_ref=faces_out.at[0], dst_ref=faces_in.at[j], send_sem=fsend_sem.at[0],
                    recv_sem=frecv_sem.at[j], device_id=(0, dom_of(j)), device_id_type=MESH,
                ).wait_recv()

            if j == 1:
                @pl.when(g == 0)
                def _():
                    face_local().wait()

        def pair(i, _, n=n, j=j, h=h):
            for k in range(2):
                q = 2 * i + k
                at = pl.multiple_of(q * LANES, LANES)
                gather_block(send_ref, n * list_size + at, low_table if h == 0 else table, tmp.at[k])
                block = tmp[k].T[:TR]
                if h == 0:
                    face = faces_in[j, pl.ds(q, 1), :]
                    block = functools.reduce(
                        lambda x, y: x + y,
                        [jnp.where(face == float(f), block[f * LOW : (f + 1) * LOW], 0.0) for f in range(FACES)],
                    )
                    sbuf[n, 0:LOW, pl.ds(at, LANES)] = block
                else:
                    sbuf[n, :, pl.ds(at, LANES)] = block
            return 0

        lax.fori_loop(0, blocks // 2, pair, 0)
        if before is not None:
            for_send(*before, lambda copy: copy.start(), lambda copy: copy.start())
        before = (j, h)
    for_send(*before, lambda copy: copy.start(), lambda copy: copy.start())

    @pl.when(g == 0)
    def _():
        for j in RELAYED:
            relay_in(j).wait_recv()
            relay_out(j).start()

    def volume_step(b, _):
        block = bucket.at[b]
        pieces = split(block[...])
        geo_ref[b] = block[0:GROWS, :]
        derivs[...] = dot3((dx_h[...], dx_l[...]), pieces, ((1,), (0,)))
        for c in range(COMPS):
            q1, x1, q2, x2 = CURL[c]
            total = None
            for a in range(3):
                for q, x, sign in ((q1, x1, 1), (q2, x2, -1)):
                    m = block[METRIC + 3 * a + x : METRIC + 3 * a + x + 1, :]
                    at = (a * COMPS + q) * DP
                    term = m * derivs[at : at + DP, :]
                    total = term if total is None else (total + term if sign > 0 else total - term)
            vol_ref[b, c * DP : (c + 1) * DP, :] = total
        for f in range(FACES):
            w = tuple(x[f * TR : (f + 1) * TR, :] for x in (tr_h, tr_l))
            own_ref[b, f] = dot3(w, pieces, ((1,), (0,)))
        return 0

    lax.fori_loop(0, groups, volume_step, 0)

    lists = 3 * groups
    far_ref[lists * list_size : lists * list_size + 8, :] = jnp.zeros((8, LANES), F32)
    fill = jnp.zeros((LANES - TR, LANES), F32)

    @pl.when(g != 0)
    def _():
        weight_copy(1, 1).wait_recv()

    def put(l, q, block):
        far_ref[l * list_size + q * LANES : l * list_size + (q + 1) * LANES, :] = jnp.concatenate([block, fill], 0).T

    def got(j, s, rows):
        l = j * groups + s
        return pltpu.make_async_remote_copy(
            src_ref=sbuf.at[l, pl.ds(0, rows)], dst_ref=arrived.at[l, pl.ds(0, rows)], send_sem=ssem.at[l],
            recv_sem=rsem.at[l], device_id=(s, dom_of(j)), device_id_type=MESH,
        )

    for j, s in [(j, s) for j in (2, 0, 1) for s in (0, 1, 2, 3)]:
        l = j * groups + s
        first = g == 0
        rest = g != 0
        if j == 1:
            @pl.when(g == s)
            def _(s=s):
                local_copy(s, LOW if s == 0 else TR).wait()

            first = jnp.logical_and(first, g != s)
            rest = jnp.logical_and(rest, g != s)

        @pl.when(first)
        def _(j=j, s=s):
            got(j, s, LOW).wait_recv()

        @pl.when(rest)
        def _(j=j, s=s):
            got(j, s, CODED if s == 0 else TR).wait_recv()

        @pl.when(g == 0)
        def _(l=l):
            gap = jnp.zeros((PP - N1, LANES), F32)
            for q in range(blocks):
                x = arrived[l, 0:LOW, q * LANES : (q + 1) * LANES]
                parts = []
                for c in range(COMPS):
                    parts += [x[c * N1 : (c + 1) * N1], gap]
                put(l, q, jnp.concatenate(parts, 0))

        @pl.when(g != 0)
        def _(l=l, s=s):
            for q in range(blocks):
                if s == 0:
                    x = arrived[l, 0:CODED, q * LANES : (q + 1) * LANES]
                    spread = dot3(split(t1x[...]), split(x), ((0,), (0,)))
                    face = x[LOW : LOW + 1, :]
                    put(l, q, functools.reduce(
                        lambda u, v: u + v,
                        [jnp.where(face == float(f), spread[f * LANES : f * LANES + TR], 0.0) for f in range(FACES)],
                    ))
                else:
                    put(l, q, arrived[l, :, q * LANES : (q + 1) * LANES])

    for i in range(groups - 1):
        for_goal(i, lambda copy: copy.wait_send())
    for j, h in order:
        for_send(j, h, lambda copy: copy.wait_send(), lambda copy: None)

    @pl.when(g == 0)
    def _():
        for j in RELAYED:
            relay_out(j).wait_send()
        for kind in range(2):
            for h in range(1, groups):
                weight_copy(kind, h).wait_send()
        for s in range(groups):
            for j in range(3):
                if (s, j) != (0, 1):
                    face_copy(s, j).wait_send()


def cross_of(u, v):
    return [u[1] * v[2] - u[2] * v[1], u[2] * v[0] - u[0] * v[2], u[0] * v[1] - u[1] * v[0]]


def final_kernel(groups, cap, recv_ref, table, own_ref, vol_ref, geo_ref, lift_ref, out_ref, tmp, far, flux):
    slots = groups * cap
    lift = split(lift_ref[...])

    for g in range(groups):

        def one_face(f, _):
            for q in range(cap // LANES):
                gather_block(recv_ref, f * slots + g * cap + q * LANES, table, tmp.at[q % 2])
                far[f, :, q * LANES : (q + 1) * LANES] = tmp[q % 2].T[:TR]
            return 0

        lax.fori_loop(0, FACES, one_face, 0)
        for f in range(FACES):
            jump = far[f] - own_ref[g, f]
            jumps = [jump[c * PP : (c + 1) * PP, :] for c in range(COMPS)]
            n = [geo_ref[g, NORMAL + c * FACES + f : NORMAL + c * FACES + f + 1, :] for c in range(3)]
            s = 0.5 * geo_ref[g, SCALE + f : SCALE + f + 1, :]
            je, jh = jumps[:3], jumps[3:]
            ne = n[0] * je[0] + n[1] * je[1] + n[2] * je[2]
            nh = n[0] * jh[0] + n[1] * jh[1] + n[2] * jh[2]
            th, te = cross_of(n, jh), cross_of(n, je)
            for c in range(3):
                flux[c, f * PP : (f + 1) * PP, :] = s * (th[c] + je[c] - n[c] * ne)
                flux[3 + c, f * PP : (f + 1) * PP, :] = s * (jh[c] - te[c] - n[c] * nh)
        for c in range(COMPS):
            result = dot3(lift, split(flux[c]), ((1,), (0,))) + vol_ref[g, c * DP : (c + 1) * DP, :]
            out_ref[c * NPM : (c + 1) * NPM, g * cap : (g + 1) * cap] = result[:NPM]


def local(groups, doms, fields, metric, normals, fscale, orders, slots, send_faces, recv_faces, dmat, tmat, lmat):
    elements = fields.shape[1]
    cap = elements // 2
    total = groups * cap
    lists = 3 * groups
    list_size = send_faces.shape[0] // lists
    blocks = list_size // LANES
    dma = pltpu.SemaphoreType.DMA
    received, own, vol, geo, lift = pl.pallas_call(
        functools.partial(move_kernel, groups, doms, cap, list_size),
        out_shape=(
            jax.ShapeDtypeStruct((lists * list_size + 8, LANES), F32),
            jax.ShapeDtypeStruct((groups, FACES, TR, cap), F32),
            jax.ShapeDtypeStruct((groups, COMPS * DP, cap), F32),
            jax.ShapeDtypeStruct((groups, GROWS, cap), F32),
            jax.ShapeDtypeStruct((DP, FACES * PP), F32),
        ),
        in_specs=[SM] + [VM] * 10,
        out_specs=(VM,) * 5,
        scratch_shapes=[
            pltpu.VMEM((ROWS, elements), F32),
            pltpu.VMEM((groups - 1, ROWS, cap), F32),
            pltpu.VMEM((groups, ROWS, cap), F32),
            pltpu.VMEM((FACES * total + 8, LANES), F32),
            pltpu.VMEM((FACES * total + 8, LANES), F32),
            pltpu.VMEM((2, LANES, LANES), F32),
            pltpu.VMEM((lists, TR, list_size), F32),
            pltpu.VMEM((lists, TR, list_size), F32),
            pltpu.VMEM((len(RELAYED), TR, list_size), F32),
            pltpu.VMEM((5, LANES, LANES), F32),
            pltpu.VMEM((2 * FACES * LANES, ROWS), BF16),
            pltpu.VMEM((2 * FACES * LANES, ROWS), BF16),
            pltpu.VMEM((FACES * TR, ROWS), BF16),
            pltpu.VMEM((FACES * TR, ROWS), BF16),
            pltpu.VMEM((3 * COMPS * DP, ROWS), BF16),
            pltpu.VMEM((3 * COMPS * DP, ROWS), BF16),
            pltpu.VMEM((3 * COMPS * DP, cap), F32),
            pltpu.VMEM((FACES * LOW, LANES), F32),
            pltpu.VMEM((CODED, FACES * LANES), F32),
            pltpu.VMEM((lists, 8, LANES), F32),
            pltpu.VMEM((3, 8, LANES), F32),
            dma((groups - 1,)),
            dma((groups,)),
            dma((lists,)),
            dma((lists,)),
            dma((len(RELAYED),)),
            dma((len(RELAYED),)),
            dma((groups,)),
            dma((1,)),
            dma((groups,)),
            dma((1,)),
            dma((lists,)),
            dma((3,)),
        ],
        compiler_params=pltpu.CompilerParams(
            vmem_limit_bytes=40 * 1024 * 1024, collective_id=0, has_side_effects=True
        ),
        name="move",
    )(
        send_faces,
        orders.reshape(-1, LANES),
        slots.reshape(-1, LANES),
        fields,
        metric,
        normals,
        fscale,
        recv_faces.reshape(-1, LANES),
        dmat[0],
        tmat[0],
        lmat[0],
    )
    return pl.pallas_call(
        functools.partial(final_kernel, groups, cap),
        out_shape=jax.ShapeDtypeStruct((COMPS * NPM, total), F32),
        in_specs=[SM, VM, VM, VM, VM, VM],
        out_specs=VM,
        scratch_shapes=[
            pltpu.VMEM((2, LANES, LANES), F32),
            pltpu.VMEM((FACES, TR, cap), F32),
            pltpu.VMEM((COMPS, FACES * PP, cap), F32),
        ],
        compiler_params=pltpu.CompilerParams(vmem_limit_bytes=24 * 1024 * 1024),
        name="final",
    )(recv_faces, received, own, vol, geo, lift)


def solution(mesh):
    col = P(None, ("grp", "dom"))
    row = P(("grp", "dom"))
    mat = P("grp", None, None)
    in_specs = (col, col, col, col, row, row, row, row, mat, mat, mat)
    body = functools.partial(local, mesh.shape["grp"], mesh.shape["dom"])
    return jax.shard_map(body, mesh=mesh, in_specs=in_specs, out_specs=col, check_vma=False)
```

```python
import functools

import jax
import jax.numpy as jnp
from jax import lax
from jax.experimental import pallas as pl
from jax.experimental.pallas import tpu as pltpu
from jax.sharding import PartitionSpec as P

NPM = 35
FPTS = 15
COMPS = 6
FACES = 4
PP = 16
DP = 40
LANES = 128
TR = COMPS * PP
NODES = (4, 10, 20, 35)
STARTS = (0, 4, 10, 20)
N1 = NODES[0]
LOW = COMPS * N1
CODED = (32, 64)
SHARE = 72
TOGETHER = 4
METRIC, NORMAL, SCALE, ONE, GEO = 0, 9, 21, 25, 26
GROWS = 32
ROWS = 240
SENT = tuple(-(-(GEO + COMPS * n) // 8) * 8 for n in NODES)
BASES = tuple(GEO + COMPS * s for s in STARTS)
RELAYED = (2, 0)
MESH = pl.DeviceIdType.MESH
F32 = jnp.float32
BF16 = jnp.bfloat16
EXACT = lax.Precision.HIGHEST


def split(x):
    high = x.astype(BF16)
    low = (x - high.astype(F32)).astype(BF16)
    return high, low


def dot3(a, b, dims):
    ah, al = a
    bh, bl = b

    def mul(x, y):
        return lax.dot_general(x, y, (dims, ((), ())), preferred_element_type=F32)

    return mul(ah, bh) + (mul(ah, bl) + mul(al, bh))


def exact_dot(a, b, dims=((1,), (0,))):
    return lax.dot_general(a, b, (dims, ((), ())), precision=EXACT, preferred_element_type=F32)


def iotas(shape):
    return lax.broadcasted_iota(jnp.int32, shape, 0), lax.broadcasted_iota(jnp.int32, shape, 1)


def ones_where(cond):
    return jnp.where(cond, 1.0, 0.0).astype(F32)


VM = pl.BlockSpec(memory_space=pltpu.VMEM)
HB = pl.BlockSpec(memory_space=pltpu.HBM)


def gather_block(index_ref, q, table, tmp):
    for i in range(LANES):
        tmp[i : i + 1, :] = table[pl.ds(index_ref[q, i], 1), :]


def flat_row(block):
    return jnp.concatenate([block[i : i + 1, :] for i in range(block.shape[0])], axis=1)


CURL = ((5, 1, 4, 2), (3, 2, 5, 0), (4, 0, 3, 1), (1, 2, 2, 1), (2, 0, 0, 2), (0, 1, 1, 0))


def place(c, shape):
    i, r = iotas(shape)
    target = BASES[3] + c * (NODES[3] - STARTS[3]) + (i - STARTS[3])
    for b in (2, 1, 0):
        width = NODES[b] - STARTS[b]
        target = jnp.where(i < NODES[b], BASES[b] + c * width + (i - STARTS[b]), target)
    return i, r, target


def coded_rows(s, shape, dim):
    i = lax.broadcasted_iota(jnp.int32, shape, dim)
    comp, node = i // N1, i & (N1 - 1)
    if s:
        width = NODES[1] - NODES[0]
        k = i - LOW
        late = (k * 43) // 256
        comp = jnp.where(i < LOW, comp, late)
        node = jnp.where(i < LOW, node, NODES[0] + k - late * width)
    return comp, node, i < COMPS * NODES[s]


def move_kernel(
    groups, doms, cap, list_size,
    send_hbm, orders_hbm, slots_hbm, fields_hbm, metric_hbm, normals_hbm, fscale_hbm, recv_hbm, dmat_hbm, tmat_hbm, lmat_hbm,
    far_ref, own_ref, vol_ref, geo_ref, lift_ref, recv_ref,
    orders_ref, slots_ref, fields_ref, metric_ref, normals_ref, fscale_ref, dmat_ref, tmat_ref, lmat_ref, send_ref, index, in_sem, index_sem,
    pay, bsend, bucket, brelay, table, low_table, tmp, sbuf, arrived, relay, wide, wcat_h, wcat_l, tr_h, tr_l, dx_h, dx_l,
    tx_h, tx_l, derivs, l1x, lift_out, lift_in, trace_out, trace_in, faces_out, faces_in,
    bsend_sem, brecv_sem, hop_sem, ssem, rsem, relay_send, relay_recv, l_send, l_recv, t_send, t_recv, fsend_sem, frecv_sem,
):
    g = lax.axis_index("grp")
    p = lax.axis_index("dom")
    slots = groups * cap
    blocks = list_size // LANES
    pairs = blocks // 2
    elements = 2 * cap
    barrier = pltpu.get_barrier_semaphore()
    loads = [
        pltpu.make_async_copy(src, dst, in_sem.at[k])
        for k, (src, dst) in enumerate(
            (
                (fields_hbm, fields_ref), (orders_hbm, orders_ref), (slots_hbm, slots_ref), (metric_hbm, metric_ref),
                (normals_hbm, normals_ref), (fscale_hbm, fscale_ref), (tmat_hbm, tmat_ref), (lmat_hbm, lmat_ref),
                (dmat_hbm, dmat_ref), (recv_hbm, recv_ref), (send_hbm, send_ref),
            )
        )
    ]
    for load in loads:
        load.start()

    def dom_of(j):
        return lax.rem(p + j - 1 + doms, doms)

    for b in range(groups):
        bucket[b, SENT[0] : ROWS, :] = jnp.zeros((ROWS - SENT[0], cap), F32)
    for j in (1, 2, 0):
        for d in range(groups):
            if (j, d) != (1, 0):
                pl.semaphore_signal(
                    barrier, inc=1, device_id=(lax.rem(g + d, groups), dom_of(j)), device_id_type=MESH
                )

    wide[...] = jnp.zeros_like(wide)
    pay[ONE : ONE + 1, :] = jnp.ones((1, elements), F32)
    pay[GEO + COMPS * NPM : ROWS, :] = jnp.zeros((ROWS - GEO - COMPS * NPM, elements), F32)
    for load in loads[:6]:
        load.wait()
    pay[METRIC : METRIC + 9, :] = metric_ref[...]
    pay[NORMAL : NORMAL + 12, :] = normals_ref[...]
    pay[SCALE : SCALE + 4, :] = fscale_ref[...]
    for b in range(4):
        width = NODES[b] - STARTS[b]
        for c in range(COMPS):
            at = BASES[b] + c * width
            pay[at : at + width, :] = fields_ref[c * NPM + STARTS[b] : c * NPM + NODES[b], :]
    target = flat_row((orders_ref[...] - 1) * cap + slots_ref[...])
    high, low = split(pay[...])
    both = jnp.concatenate([high, low], axis=0)
    step = min(cap, 256)

    def build(h, dst):
        for k in range(0, cap, step):
            ids = lax.broadcasted_iota(jnp.int32, (step, elements), 0) + (h * cap + k)
            hot = jnp.where(ids == target, 1.0, 0.0).astype(BF16)
            out = lax.dot_general(both, hot, (((1,), (1,)), ((), ())), preferred_element_type=F32)
            dst[:, k : k + step] = out[:ROWS] + out[ROWS:]

    def goal(i):
        top = groups - 1 - i
        return top - jnp.where(top <= g, 1, 0)

    def bucket_copy(i, rows):
        return pltpu.make_async_remote_copy(
            src_ref=bsend.at[i, pl.ds(0, rows)],
            dst_ref=bucket.at[g, pl.ds(0, rows)],
            send_sem=bsend_sem.at[i],
            recv_sem=brecv_sem.at[g],
            device_id=(goal(i), p),
            device_id_type=MESH,
        )

    main = ROWS - SHARE

    def hop_in():
        return pltpu.make_async_remote_copy(
            src_ref=bsend.at[0, pl.ds(main, SHARE)], dst_ref=brelay, send_sem=hop_sem.at[0], recv_sem=hop_sem.at[1],
            device_id=(2, p), device_id_type=MESH,
        )

    def hop_out():
        return pltpu.make_async_remote_copy(
            src_ref=brelay, dst_ref=bucket.at[0, pl.ds(main, SHARE)], send_sem=hop_sem.at[2], recv_sem=hop_sem.at[3],
            device_id=(3, p), device_id_type=MESH,
        )

    def for_goal(i, act):
        for h in (groups - 1 - i, groups - 2 - i):
            hit = goal(i) == h
            if i == 0 and h == groups - 1:
                @pl.when(g == 0)
                def _():
                    act(hop_in())
                    act(bucket_copy(0, main))

                hit = jnp.logical_and(hit, g != 0)

            @pl.when(hit)
            def _(h=h):
                act(bucket_copy(i, SENT[h]))

    build(goal(0), bsend.at[0])
    pl.semaphore_wait(barrier, 3 * groups - 1)
    for i in range(1, groups - 1):
        build(goal(i), bsend.at[i])
        for_goal(i - 1, lambda copy: copy.start())
    build(g, bucket.at[g])
    for_goal(groups - 2, lambda copy: copy.start())

    for load in loads[6:]:
        load.wait()

    def fetch(n, q):
        return pltpu.make_async_copy(send_ref.at[n * pairs + q], index.at[q], index_sem.at[q])

    own_nodes = (g + 2) * (g + 3) * (g + 4) // 6
    wide[0, 0:NPM, 0 : FPTS * FACES] = tmat_ref[:, 0, :]
    wide[1, 0:NPM, 0 : FPTS * FACES] = lmat_ref[:, 0, :]
    wide[2, 0:NPM, 0 : 3 * NPM] = dmat_ref[:, 0, :]
    i, r = iotas((FACES * PP, LANES))
    order_points = ones_where((r == (i & (PP - 1)) * FACES + (i // PP)) & ((i & (PP - 1)) < FPTS))
    trace = exact_dot(order_points, wide[0], ((1,), (1,)))
    lift = exact_dot(wide[1, 0:DP], order_points, ((1,), (1,)))
    row = lax.broadcasted_iota(jnp.int32, (DP, FACES * PP), 0)
    lift = jnp.where(row < own_nodes, lift, 0.0)

    def weight_copy(kind, h):
        src, dst, send, recv = (
            (lift_out, lift_in, l_send, l_recv.at[0]),
            (trace_out, trace_in.at[0], t_send, t_recv.at[0]),
            (trace_out, trace_in.at[1], t_send, t_recv.at[1]),
        )[kind]
        return pltpu.make_async_remote_copy(
            src_ref=src, dst_ref=dst, send_sem=send.at[h], recv_sem=recv, device_id=(h, p), device_id_type=MESH
        )

    trace_out[...] = trace
    lift_out[...] = jnp.zeros((8, LANES), F32)
    lift_out[:, 0 : FACES * PP] = lift[0:8]

    tr_f = [[] for _ in range(FACES)]
    node = lax.broadcasted_iota(jnp.int32, (NPM, ROWS), 0)
    for at in range(0, 3 * COMPS * DP, DP):
        dx_h[at + DP - 8 : at + DP, :] = jnp.zeros((8, ROWS), BF16)
        dx_l[at + DP - 8 : at + DP, :] = jnp.zeros((8, ROWS), BF16)
    for c in range(COMPS):
        i, r, at = place(c, (LANES, ROWS))
        spread = ones_where((r == at) & (i < own_nodes) & (i < NPM))
        part = exact_dot(trace, spread)
        for f in range(FACES):
            tr_f[f].append(part[f * PP : (f + 1) * PP])
        block = exact_dot(wide[2], spread, ((0,), (0,)))
        for a in range(3):
            piece = split(jnp.where(node < own_nodes, block[a * NPM : (a + 1) * NPM], 0.0))
            at_row = (a * COMPS + c) * DP
            dx_h[at_row : at_row + NPM, :] = piece[0]
            dx_l[at_row : at_row + NPM, :] = piece[1]
    tr_f = [jnp.concatenate(parts + [jnp.zeros((LANES - TR, ROWS), F32)], 0) for parts in tr_f]

    def face_copy(s, j):
        return pltpu.make_async_remote_copy(
            src_ref=faces_out.at[j * groups + s],
            dst_ref=faces_in.at[j],
            send_sem=fsend_sem.at[j * groups + s],
            recv_sem=frecv_sem.at[j],
            device_id=(s, lax.rem(p - j + 1 + doms, doms)),
            device_id_type=MESH,
        )

    def face_local():
        return pltpu.make_async_copy(faces_out.at[groups], faces_in.at[1], frecv_sem.at[1])

    @pl.when(g == 0)
    def _():
        lift_in[...] = lift_out[...]
        for kind in range(2):
            for h in range(1, groups):
                weight_copy(kind, h).start()
        rows = slots // LANES
        count = -(-(3 * groups * blocks) // 8) * 8
        found = jnp.zeros((count, LANES), F32)
        per = recv_ref.shape[1]
        for f in range(1, FACES):
            entry = jnp.concatenate(
                [flat_row(recv_ref[k]) for k in range(f * rows // per, (f + 1) * rows // per)], axis=1
            )
            upper, lower = entry // LANES, entry & (LANES - 1)
            a = jnp.where(lax.broadcasted_iota(jnp.int32, (count, slots), 0) == upper, float(f), 0.0).astype(BF16)
            b = jnp.where(lax.broadcasted_iota(jnp.int32, (LANES, slots), 0) == lower, 1.0, 0.0).astype(BF16)
            found = found + lax.dot_general(a, b, (((1,), (1,)), ((), ())), preferred_element_type=F32)
        for n in range(3 * groups):
            faces_out[n, 0:blocks, :] = found[n * blocks : (n + 1) * blocks]
        for s in range(groups):
            for j in range(3):
                (face_local() if (s, j) == (0, 1) else face_copy(s, j)).start()

    @pl.when(g == 1)
    def _():
        trace_in[1] = trace_out[...]
        for h in range(2, groups):
            weight_copy(2, h).start()

    @pl.when(g != 0)
    def _():
        weight_copy(0, 1).wait_recv()

    i, r = iotas((LOW, 8))
    picked = exact_dot(ones_where(r == (i & (N1 - 1))), lift_in[...])
    for f in range(FACES):
        i, r = iotas((LANES, LANES))
        fan = ones_where(i == f * PP + (r & (PP - 1)))
        i, r = iotas((LOW, LANES))
        l1x[f * LOW : (f + 1) * LOW, :] = jnp.where((r // PP) == (i // N1), exact_dot(picked, fan), 0.0)

    for f in range(FACES):
        at = f * 2 * LANES
        for k, piece in enumerate(split(tr_f[f])):
            (tr_h, tr_l)[k][f * TR : (f + 1) * TR, :] = piece[:TR]
            (wcat_h, wcat_l)[k][at : at + LANES, :] = piece
        lowered = exact_dot(l1x[...], tr_f[f])
        filled = jnp.concatenate([lowered, jnp.zeros((LANES - TR, ROWS), F32)], 0)
        for k, piece in enumerate(split(filled)):
            (wcat_h, wcat_l)[k][at + LANES : at + 2 * LANES, :] = piece

        @pl.when(g < 2)
        def _(f=f, at=at):
            used = COMPS * own_nodes
            i, r = iotas((LANES, ROWS))
            coded = jnp.where((i < used) & (r == GEO + i), 1.0, 0.0) + jnp.where((i == used) & (r == ONE), float(f), 0.0)
            wcat_h[at : at + LANES, :] = coded.astype(BF16)
            wcat_l[at : at + LANES, :] = jnp.zeros((LANES, ROWS), BF16)

        @pl.when(g == 0)
        def _(f=f, lowered=lowered):
            i, r = iotas((TR, TR))
            pick = ones_where(((i & (PP - 1)) < N1) & (r == f * LOW + (i // PP) * N1 + (i & (PP - 1))))
            for k, piece in enumerate(split(exact_dot(pick, lowered))):
                (tr_h, tr_l)[k][f * TR : (f + 1) * TR, :] = piece

    i, r = iotas((DP, FACES * PP))
    unit = ones_where((i < N1) & ((r & (PP - 1)) == i))
    lift_ref[...] = jnp.zeros_like(lift_ref)
    for c in range(TOGETHER):
        lift_ref[c * DP : (c + 1) * DP, c * FACES * PP : (c + 1) * FACES * PP] = jnp.where(g == 0, unit, lift)

    for t in (table, low_table):
        t[FACES * slots : FACES * slots + 8, :] = jnp.zeros((8, LANES), F32)

    def make_tables(b):
        coefs = split(bucket[b].T)
        for f in range(FACES):
            w = tuple(x[f * 2 * LANES : (f + 1) * 2 * LANES, :] for x in (wcat_h, wcat_l))
            rows = dot3(coefs, w, ((1,), (1,)))
            at = pl.multiple_of(f * slots + b * cap, LANES)
            table[pl.ds(at, cap), :] = rows[:, :LANES]
            low_table[pl.ds(at, cap), :] = rows[:, LANES:]

    def arrival(b, rows):
        return pltpu.make_async_remote_copy(
            src_ref=bsend.at[0, pl.ds(0, rows)], dst_ref=bucket.at[b, pl.ds(0, rows)], send_sem=bsend_sem.at[0],
            recv_sem=brecv_sem.at[b], device_id=(b, p), device_id_type=MESH,
        )

    def arrive(b):
        for h in range(groups):
            hit = g == h
            if h == groups - 1:
                @pl.when(jnp.logical_and(hit, b == 0))
                def _():
                    arrival(b, main).wait_recv()
                    hop_out().wait_recv()

                hit = jnp.logical_and(hit, b != 0)

            @pl.when(hit)
            def _(h=h):
                arrival(b, SENT[h]).wait_recv()

    @pl.when(g == 2)
    def _():
        hop_in().wait_recv()
        hop_out().start()

    def table_step(k, _):
        b = lax.rem(g - k + groups, groups)

        @pl.when(k > 0)
        def _():
            arrive(b)

        make_tables(b)
        return 0

    lax.fori_loop(0, groups, table_step, 0)

    def list_copy(j, h, rows):
        n = j * groups + h
        return pltpu.make_async_remote_copy(
            src_ref=sbuf.at[n, pl.ds(0, rows)], dst_ref=arrived.at[j * groups + g, pl.ds(0, rows)], send_sem=ssem.at[n],
            recv_sem=rsem.at[j * groups + g], device_id=(h, dom_of(j)), device_id_type=MESH,
        )

    def local_copy(h, rows):
        n = groups + h
        return pltpu.make_async_copy(sbuf.at[n, pl.ds(0, rows)], arrived.at[n, pl.ds(0, rows)], rsem.at[n])

    def relay_in(k):
        j = RELAYED[k]
        n = j * groups + 1
        return pltpu.make_async_remote_copy(
            src_ref=sbuf.at[n], dst_ref=relay.at[k], send_sem=ssem.at[n], recv_sem=relay_recv.at[k],
            device_id=(0, p), device_id_type=MESH,
        )

    def relay_out(k):
        j = RELAYED[k]
        return pltpu.make_async_remote_copy(
            src_ref=relay.at[k], dst_ref=arrived.at[j * groups + 2], send_sem=relay_send.at[k],
            recv_sem=rsem.at[j * groups + 2], device_id=(1, dom_of(j)), device_id_type=MESH,
        )

    def width_cases():
        return ((g == 0, CODED[0]), (g == 1, CODED[1]), (g >= 2, TR))

    def for_list(j, h, act, act_local):
        here = jnp.logical_and(j == 1, h == g)
        hop = jnp.logical_and(jnp.logical_and(g == 2, h == 1), j != 1)
        plain = jnp.logical_not(jnp.logical_or(here, hop))
        for hit, rows in width_cases():
            @pl.when(jnp.logical_and(hit, plain))
            def _(rows=rows):
                act(list_copy(j, h, rows))

            @pl.when(jnp.logical_and(hit, here))
            def _(rows=rows):
                act_local(local_copy(h, rows))
        for k in range(len(RELAYED)):
            @pl.when(jnp.logical_and(hop, j == RELAYED[k]))
            def _(k=k):
                act(relay_in(k))

    def for_low(j, act, act_local):
        here = jnp.logical_and(j == 1, g == 0)

        @pl.when(jnp.logical_not(here))
        def _():
            act(list_copy(j, 0, LOW))

        @pl.when(here)
        def _():
            act_local(local_copy(0, LOW))

    def turn(k):
        return jnp.where(k == 0, 2, k - 1)

    def which(k):
        pos = lax.rem(k, 3)
        first = 3 - jnp.where(g == 3, 1, jnp.where(g == 2, 2, 0))
        second = jnp.where(g == 3, 1, jnp.where(g == 2, 3, 2))
        third = jnp.maximum(g, 1)
        return turn(k // 3), jnp.where(pos == 0, first, jnp.where(pos == 1, second, third))

    def start(copy):
        copy.start()

    many = 3 * (groups - 1)

    def numbers(k):
        j, h = which(jnp.minimum(k, many - 1))
        return jnp.where(k < many, j * groups + h, turn(jnp.maximum(k - many, 0)) * groups)

    for q in range(pairs):
        fetch(numbers(0), q).start()

    def one_list(k, _):
        j, h = which(k)
        n = j * groups + h
        ahead = numbers(k + 1)
        for q in range(blocks):
            if q % 2 == 0:
                fetch(n, q // 2).wait()
            gather_block(index.at[q // 2], q % 2, table, tmp.at[q % 2])
            if q % 2:
                fetch(ahead, q // 2).start()
            sbuf[n, :, q * LANES : (q + 1) * LANES] = tmp[q % 2].T[:TR]
            if q == 1:
                @pl.when(k > 0)
                def _():
                    for_list(*which(k - 1), start, start)
        return 0

    lax.fori_loop(0, many, one_list, 0)

    def low_list(k, _):
        j = turn(k)
        n = j * groups
        ahead = turn(k + 1) * groups

        @pl.when(jnp.logical_or(g != 0, j != 1))
        def _():
            pltpu.make_async_remote_copy(
                src_ref=faces_out.at[0], dst_ref=faces_in.at[j], send_sem=fsend_sem.at[0],
                recv_sem=frecv_sem.at[j], device_id=(0, dom_of(j)), device_id_type=MESH,
            ).wait_recv()

        @pl.when(jnp.logical_and(g == 0, j == 1))
        def _():
            face_local().wait()

        for q in range(blocks):
            if q % 2 == 0:
                fetch(n, q // 2).wait()
            gather_block(index.at[q // 2], q % 2, low_table, tmp.at[q % 2])
            if q % 2:
                @pl.when(k < 2)
                def _(q=q):
                    fetch(ahead, q // 2).start()

            block = tmp[q % 2].T[:TR]
            face = faces_in[j, q : q + 1, :]
            sbuf[n, 0:LOW, q * LANES : (q + 1) * LANES] = functools.reduce(
                lambda x, y: x + y,
                [jnp.where(face == float(f), block[f * LOW : (f + 1) * LOW], 0.0) for f in range(FACES)],
            )
            if q == 1:
                @pl.when(k == 0)
                def _():
                    for_list(*which(many - 1), start, start)

                @pl.when(k > 0)
                def _():
                    for_low(turn(k - 1), start, start)
        return 0

    lax.fori_loop(0, 3, low_list, 0)
    for_low(turn(2), start, start)

    def volume_step(b, _):
        block = bucket.at[b]
        pieces = split(block[...])
        geo_ref[b] = block[0:GROWS, :]
        derivs[...] = dot3((dx_h[...], dx_l[...]), pieces, ((1,), (0,)))
        for c in range(COMPS):
            q1, x1, q2, x2 = CURL[c]
            total = None
            for a in range(3):
                for q, x, sign in ((q1, x1, 1), (q2, x2, -1)):
                    m = block[METRIC + 3 * a + x : METRIC + 3 * a + x + 1, :]
                    at = (a * COMPS + q) * DP
                    term = m * derivs[at : at + DP, :]
                    total = term if total is None else (total + term if sign > 0 else total - term)
            vol_ref[b, c * DP : (c + 1) * DP, :] = total
        for f in range(FACES):
            w = tuple(x[f * TR : (f + 1) * TR, :] for x in (tr_h, tr_l))
            own_ref[b, f] = dot3(w, pieces, ((1,), (0,)))
        return 0

    lax.fori_loop(0, groups, volume_step, 0)

    @pl.when(g != 0)
    def _():
        weight_copy(1, 1).wait_recv()

        @pl.when(g > 1)
        def _():
            weight_copy(2, 2).wait_recv()

        for s in range(2):
            for f in range(FACES):
                i, r = iotas((TR, FACES * PP))
                fan = ones_where(r == f * PP + (i & (PP - 1)))
                _, at_node, _ = coded_rows(s, (CODED[s], LANES), 0)
                _, r = iotas((CODED[s], LANES))
                rows = exact_dot(exact_dot(fan, trace_in[s]), ones_where(r == at_node), ((1,), (1,)))
                comp, _, valid = coded_rows(s, (TR, CODED[s]), 1)
                i, _ = iotas((TR, CODED[s]))
                pieces = split(jnp.where(((i // PP) == comp) & valid, rows, 0.0))
                tx_h[s, f * TR : (f + 1) * TR, 0 : CODED[s]] = pieces[0]
                tx_l[s, f * TR : (f + 1) * TR, 0 : CODED[s]] = pieces[1]

    @pl.when(g == 0)
    def _():
        for k in range(len(RELAYED)):
            relay_in(k).wait_recv()
            relay_out(k).start()

    lists = 3 * groups
    far_ref[lists * list_size : lists * list_size + 8, :] = jnp.zeros((8, LANES), F32)
    fill = jnp.zeros((LANES - TR, LANES), F32)

    def got(l, j, s, rows):
        return pltpu.make_async_remote_copy(
            src_ref=sbuf.at[l, pl.ds(0, rows)], dst_ref=arrived.at[l, pl.ds(0, rows)], send_sem=ssem.at[l],
            recv_sem=rsem.at[l], device_id=(s, dom_of(j)), device_id_type=MESH,
        )

    def take(k, _):
        j = turn(k)
        for s in range(groups):
            l = j * groups + s
            rows = CODED[s] if s < 2 else TR
            here = jnp.logical_and(j == 1, g == s)
            away = jnp.logical_not(here)
            for hit, size in ((g == 0, LOW), (g != 0, rows)):
                @pl.when(jnp.logical_and(hit, away))
                def _(size=size, l=l, s=s):
                    got(l, j, s, size).wait_recv()

            @pl.when(here)
            def _(s=s, rows=rows):
                local_copy(s, rows if s else LOW).wait()

            def put(q, block, l=l):
                at = pl.multiple_of(l * list_size + q * LANES, LANES)
                far_ref[pl.ds(at, LANES), :] = jnp.concatenate([block, fill], 0).T

            @pl.when(g == 0)
            def _(l=l, put=put):
                gap = jnp.zeros((PP - N1, LANES), F32)
                for q in range(blocks):
                    x = arrived[l, 0:LOW, q * LANES : (q + 1) * LANES]
                    parts = []
                    for c in range(COMPS):
                        parts += [x[c * N1 : (c + 1) * N1], gap]
                    put(q, jnp.concatenate(parts, 0))

            @pl.when(g != 0)
            def _(l=l, s=s, put=put, rows=rows):
                if s > 1:
                    for q in range(blocks):
                        put(q, arrived[l, :, q * LANES : (q + 1) * LANES])
                    return
                used = COMPS * NODES[s]
                w = (tx_h[s, :, 0:rows], tx_l[s, :, 0:rows])
                for q in range(0, blocks, 2):
                    x = arrived[l, 0:rows, q * LANES : (q + 2) * LANES]
                    spread = dot3(w, split(x), ((1,), (0,)))
                    face = x[used : used + 1, :]
                    block = functools.reduce(
                        lambda u, v: u + v,
                        [jnp.where(face == float(f), spread[f * TR : (f + 1) * TR], 0.0) for f in range(FACES)],
                    )
                    put(q, block[:, :LANES])
                    put(q + 1, block[:, LANES:])
        return 0

    lax.fori_loop(0, 3, take, 0)

    def sent(copy):
        copy.wait_send()

    def nothing(copy):
        pass

    for i in range(groups - 1):
        for_goal(i, sent)

    def list_sent(k, _):
        j, h = which(k)
        here = jnp.logical_and(j == 1, h == g)
        for hit, rows in width_cases():
            @pl.when(jnp.logical_and(hit, jnp.logical_not(here)))
            def _(rows=rows):
                list_copy(j, h, rows).wait_send()
        return 0

    def low_sent(k, _):
        j = turn(k)

        @pl.when(jnp.logical_or(g != 0, j != 1))
        def _():
            list_copy(j, 0, LOW).wait_send()

        return 0

    lax.fori_loop(0, many, list_sent, 0)
    lax.fori_loop(0, 3, low_sent, 0)

    @pl.when(g == 2)
    def _():
        hop_out().wait_send()

    @pl.when(g == 1)
    def _():
        for h in range(2, groups):
            weight_copy(2, h).wait_send()

    @pl.when(g == 0)
    def _():
        for k in range(len(RELAYED)):
            relay_out(k).wait_send()
        for kind in range(2):
            for h in range(1, groups):
                weight_copy(kind, h).wait_send()
        for s in range(groups):
            for j in range(3):
                if (s, j) != (0, 1):
                    face_copy(s, j).wait_send()


def cross_of(u, v):
    return [u[1] * v[2] - u[2] * v[1], u[2] * v[0] - u[0] * v[2], u[0] * v[1] - u[1] * v[0]]


def final_kernel(
    groups, cap, recv_ref, table, own_ref, vol_ref, geo_ref, lift_ref, out_hbm,
    tmp, far, flux, out, index, index_sem, out_sem,
):
    slots = groups * cap
    blocks = cap // LANES
    lift = split(lift_ref[...])

    def fetch(g, f):
        return pltpu.make_async_copy(recv_ref.at[f * groups + g], index.at[f], index_sem.at[f])

    def leave(g):
        slot = lax.rem(g, 2)
        return pltpu.make_async_copy(
            out.at[slot], out_hbm.at[:, pl.ds(pl.multiple_of(g * cap, LANES), cap)], out_sem.at[slot]
        )

    for f in range(FACES):
        fetch(0, f).start()

    def part(g, _):
        for f in range(FACES):
            fetch(g, f).wait()
            for q in range(blocks):
                gather_block(index.at[f], q, table, tmp.at[q % 2])
                far[f, :, q * LANES : (q + 1) * LANES] = tmp[q % 2].T[:TR]

            @pl.when(g < groups - 1)
            def _(f=f):
                fetch(g + 1, f).start()

        for f in range(FACES):
            jump = far[f] - own_ref[g, f]
            jumps = [jump[c * PP : (c + 1) * PP, :] for c in range(COMPS)]
            n = [geo_ref[g, NORMAL + c * FACES + f : NORMAL + c * FACES + f + 1, :] for c in range(3)]
            s = 0.5 * geo_ref[g, SCALE + f : SCALE + f + 1, :]
            je, jh = jumps[:3], jumps[3:]
            ne = n[0] * je[0] + n[1] * je[1] + n[2] * je[2]
            nh = n[0] * jh[0] + n[1] * jh[1] + n[2] * jh[2]
            th, te = cross_of(n, jh), cross_of(n, je)
            for c in range(3):
                at = (c * FACES + f) * PP
                flux[at : at + PP, :] = s * (th[c] + je[c] - n[c] * ne)
                at += 3 * FACES * PP
                flux[at : at + PP, :] = s * (jh[c] - te[c] - n[c] * nh)

        @pl.when(g > 1)
        def _():
            leave(g - 2).wait()

        slot = lax.rem(g, 2)
        for c in range(0, COMPS, TOGETHER):
            count = min(TOGETHER, COMPS - c)
            deep = count * FACES * PP
            w = tuple(x[: count * DP, :deep] for x in lift)
            lifted = dot3(w, split(flux[c * FACES * PP : c * FACES * PP + deep, :]), ((1,), (0,)))
            lifted = lifted + vol_ref[g, c * DP : (c + count) * DP, :]
            for k in range(count):
                out[slot, (c + k) * NPM : (c + k + 1) * NPM, :] = lifted[k * DP : k * DP + NPM]
        leave(g).start()
        return 0

    lax.fori_loop(0, groups, part, 0)
    leave(groups - 2).wait()
    leave(groups - 1).wait()


def local(groups, doms, fields, metric, normals, fscale, orders, slots, send_faces, recv_faces, dmat, tmat, lmat):
    elements = fields.shape[1]
    cap = elements // 2
    total = groups * cap
    lists = 3 * groups
    list_size = send_faces.shape[0] // lists
    blocks = list_size // LANES
    dma = pltpu.SemaphoreType.DMA
    i32 = jnp.int32
    vmem = pltpu.VMEM
    recv_shape = (FACES * groups, cap // LANES, LANES)
    received, own, vol, geo, lift, entries = pl.pallas_call(
        functools.partial(move_kernel, groups, doms, cap, list_size),
        out_shape=(
            jax.ShapeDtypeStruct((lists * list_size + 8, LANES), F32),
            jax.ShapeDtypeStruct((groups, FACES, TR, cap), F32),
            jax.ShapeDtypeStruct((groups, COMPS * DP, cap), F32),
            jax.ShapeDtypeStruct((groups, GROWS, cap), F32),
            jax.ShapeDtypeStruct((TOGETHER * DP, TOGETHER * FACES * PP), F32),
            jax.ShapeDtypeStruct(recv_shape, i32),
        ),
        in_specs=[HB] * 11,
        out_specs=(VM,) * 6,
        scratch_shapes=[
            vmem((elements // LANES, LANES), i32),
            vmem((elements // LANES, LANES), i32),
            vmem(fields.shape, F32),
            vmem(metric.shape, F32),
            vmem(normals.shape, F32),
            vmem(fscale.shape, F32),
            vmem((NPM, 1, 3 * NPM), F32),
            vmem((NPM, 1, FPTS * FACES), F32),
            vmem((NPM, 1, FPTS * FACES), F32),
            vmem((lists * blocks // 2, 2, LANES), i32),
            pltpu.SMEM((blocks // 2, 2, LANES), i32),
            dma((11,)),
            dma((blocks // 2,)),
            vmem((ROWS, elements), F32),
            vmem((groups - 1, ROWS, cap), F32),
            vmem((groups, ROWS, cap), F32),
            vmem((SHARE, cap), F32),
            vmem((FACES * total + 8, LANES), F32),
            vmem((FACES * total + 8, LANES), F32),
            vmem((2, LANES, LANES), F32),
            vmem((lists, TR, list_size), F32),
            vmem((lists, TR, list_size), F32),
            vmem((len(RELAYED), TR, list_size), F32),
            vmem((3, LANES, LANES), F32),
            vmem((2 * FACES * LANES, ROWS), BF16),
            vmem((2 * FACES * LANES, ROWS), BF16),
            vmem((FACES * TR, ROWS), BF16),
            vmem((FACES * TR, ROWS), BF16),
            vmem((3 * COMPS * DP, ROWS), BF16),
            vmem((3 * COMPS * DP, ROWS), BF16),
            vmem((2, FACES * TR, LANES), BF16),
            vmem((2, FACES * TR, LANES), BF16),
            vmem((3 * COMPS * DP, cap), F32),
            vmem((FACES * LOW, LANES), F32),
            vmem((8, LANES), F32),
            vmem((8, LANES), F32),
            vmem((FACES * PP, LANES), F32),
            vmem((2, FACES * PP, LANES), F32),
            vmem((lists, 8, LANES), F32),
            vmem((3, 8, LANES), F32),
            dma((groups - 1,)),
            dma((groups,)),
            dma((4,)),
            dma((lists,)),
            dma((lists,)),
            dma((len(RELAYED),)),
            dma((len(RELAYED),)),
            dma((groups,)),
            dma((1,)),
            dma((groups,)),
            dma((2,)),
            dma((lists,)),
            dma((3,)),
        ],
        compiler_params=pltpu.CompilerParams(
            vmem_limit_bytes=40 * 1024 * 1024, collective_id=0, has_side_effects=True
        ),
        name="move",
    )(
        *[
            pltpu.with_memory_space_constraint(x, pltpu.HBM)
            for x in (
                send_faces.reshape(-1, 2, LANES),
                orders.reshape(-1, LANES),
                slots.reshape(-1, LANES),
                fields,
                metric,
                normals,
                fscale,
                recv_faces.reshape(recv_shape),
                jnp.transpose(dmat, (2, 0, 1)),
                jnp.transpose(tmat, (2, 0, 1)),
                jnp.transpose(lmat, (1, 0, 2)),
            )
        ]
    )
    return pl.pallas_call(
        functools.partial(final_kernel, groups, cap),
        out_shape=jax.ShapeDtypeStruct((COMPS * NPM, total), F32),
        in_specs=[VM] * 6,
        out_specs=HB,
        scratch_shapes=[
            vmem((2, LANES, LANES), F32),
            vmem((FACES, TR, cap), F32),
            vmem((COMPS * FACES * PP, cap), F32),
            vmem((2, COMPS * NPM, cap), F32),
            pltpu.SMEM((FACES, cap // LANES, LANES), i32),
            dma((FACES,)),
            dma((2,)),
        ],
        compiler_params=pltpu.CompilerParams(vmem_limit_bytes=24 * 1024 * 1024),
        name="final",
    )(entries, received, own, vol, geo, lift)


def solution(mesh):
    col = P(None, ("grp", "dom"))
    row = P(("grp", "dom"))
    mat = P("grp", None, None)
    in_specs = (col, col, col, col, row, row, row, row, mat, mat, mat)
    body = functools.partial(local, mesh.shape["grp"], mesh.shape["dom"])
    return jax.shard_map(body, mesh=mesh, in_specs=in_specs, out_specs=col, check_vma=False)
```

```python
import functools

import jax
import jax.numpy as jnp
from jax import lax
from jax.experimental import pallas as pl
from jax.experimental.pallas import tpu as pltpu
from jax.sharding import PartitionSpec as P

NPM = 35
FPTS = 15
COMPS = 6
FACES = 4
PP = 16
DP = 40
LANES = 128
TR = COMPS * PP
NODES = (4, 10, 20, 35)
STARTS = (0, 4, 10, 20)
N1 = NODES[0]
LOW = COMPS * N1
CODED = (32, 64)
SHARE = 72
TOGETHER = 4
METRIC, NORMAL, SCALE, ONE, GEO = 0, 9, 21, 25, 26
GROWS = 32
ROWS = 240
SENT = tuple(-(-(GEO + COMPS * n) // 8) * 8 for n in NODES)
BASES = tuple(GEO + COMPS * s for s in STARTS)
RELAYED = (2, 0)
MESH = pl.DeviceIdType.MESH
F32 = jnp.float32
BF16 = jnp.bfloat16
EXACT = lax.Precision.HIGHEST


def split(x):
    high = x.astype(BF16)
    low = (x - high.astype(F32)).astype(BF16)
    return high, low


def dot3(a, b, dims):
    ah, al = a
    bh, bl = b

    def mul(x, y):
        return lax.dot_general(x, y, (dims, ((), ())), preferred_element_type=F32)

    return mul(ah, bh) + (mul(ah, bl) + mul(al, bh))


def exact_dot(a, b, dims=((1,), (0,))):
    return lax.dot_general(a, b, (dims, ((), ())), precision=EXACT, preferred_element_type=F32)


def iotas(shape):
    return lax.broadcasted_iota(jnp.int32, shape, 0), lax.broadcasted_iota(jnp.int32, shape, 1)


def ones_where(cond):
    return jnp.where(cond, 1.0, 0.0).astype(F32)


VM = pl.BlockSpec(memory_space=pltpu.VMEM)
HB = pl.BlockSpec(memory_space=pltpu.HBM)


def gather_block(index_ref, q, table, tmp):
    for i in range(LANES):
        tmp[i : i + 1, :] = table[pl.ds(index_ref[q, i], 1), :]


def flat_row(block):
    return jnp.concatenate([block[i : i + 1, :] for i in range(block.shape[0])], axis=1)


CURL = ((5, 1, 4, 2), (3, 2, 5, 0), (4, 0, 3, 1), (1, 2, 2, 1), (2, 0, 0, 2), (0, 1, 1, 0))


def place(c, shape):
    i, r = iotas(shape)
    target = BASES[3] + c * (NODES[3] - STARTS[3]) + (i - STARTS[3])
    for b in (2, 1, 0):
        width = NODES[b] - STARTS[b]
        target = jnp.where(i < NODES[b], BASES[b] + c * width + (i - STARTS[b]), target)
    return i, r, target


def coded_rows(s, shape, dim):
    i = lax.broadcasted_iota(jnp.int32, shape, dim)
    comp, node = i // N1, i & (N1 - 1)
    if s:
        width = NODES[1] - NODES[0]
        k = i - LOW
        late = (k * 43) // 256
        comp = jnp.where(i < LOW, comp, late)
        node = jnp.where(i < LOW, node, NODES[0] + k - late * width)
    return comp, node, i < COMPS * NODES[s]


def move_kernel(
    groups, doms, cap, list_size,
    send_hbm, orders_hbm, slots_hbm, fields_hbm, metric_hbm, normals_hbm, fscale_hbm, recv_hbm, dmat_hbm, tmat_hbm, lmat_hbm,
    far_ref, own_ref, vol_ref, geo_ref, lift_ref, recv_ref,
    orders_ref, slots_ref, fields_ref, metric_ref, normals_ref, fscale_ref, dmat_ref, tmat_ref, lmat_ref, send_ref, in_sem,
    pay, bsend, bucket, brelay, table, low_table, tmp, sbuf, arrived, relay, wide, wcat_h, wcat_l, tr_h, tr_l, dx_h, dx_l,
    tx_h, tx_l, derivs, l1x, lift_out, lift_in, trace_out, trace_in, faces_out, faces_in,
    bsend_sem, brecv_sem, hop_sem, ssem, rsem, relay_send, relay_recv, l_send, l_recv, t_send, t_recv, fsend_sem, frecv_sem,
):
    g = lax.axis_index("grp")
    p = lax.axis_index("dom")
    slots = groups * cap
    blocks = list_size // LANES
    pairs = blocks // 2
    elements = 2 * cap
    barrier = pltpu.get_barrier_semaphore()
    loads = [
        pltpu.make_async_copy(src, dst, in_sem.at[k])
        for k, (src, dst) in enumerate(
            (
                (fields_hbm, fields_ref), (orders_hbm, orders_ref), (slots_hbm, slots_ref), (metric_hbm, metric_ref),
                (normals_hbm, normals_ref), (fscale_hbm, fscale_ref), (tmat_hbm, tmat_ref), (lmat_hbm, lmat_ref),
                (dmat_hbm, dmat_ref), (recv_hbm, recv_ref), (send_hbm, send_ref),
            )
        )
    ]
    for load in loads:
        load.start()

    def dom_of(j):
        return lax.rem(p + j - 1 + doms, doms)

    for b in range(groups):
        bucket[b, SENT[0] : ROWS, :] = jnp.zeros((ROWS - SENT[0], cap), F32)
    for j in (1, 2, 0):
        for d in range(groups):
            if (j, d) != (1, 0):
                pl.semaphore_signal(
                    barrier, inc=1, device_id=(lax.rem(g + d, groups), dom_of(j)), device_id_type=MESH
                )

    wide[...] = jnp.zeros_like(wide)
    pay[ONE : ONE + 1, :] = jnp.ones((1, elements), F32)
    pay[GEO + COMPS * NPM : ROWS, :] = jnp.zeros((ROWS - GEO - COMPS * NPM, elements), F32)
    for load in loads[:6]:
        load.wait()
    pay[METRIC : METRIC + 9, :] = metric_ref[...]
    pay[NORMAL : NORMAL + 12, :] = normals_ref[...]
    pay[SCALE : SCALE + 4, :] = fscale_ref[...]
    for b in range(4):
        width = NODES[b] - STARTS[b]
        for c in range(COMPS):
            at = BASES[b] + c * width
            pay[at : at + width, :] = fields_ref[c * NPM + STARTS[b] : c * NPM + NODES[b], :]
    target = flat_row((orders_ref[...] - 1) * cap + slots_ref[...])
    high, low = split(pay[...])
    both = jnp.concatenate([high, low], axis=0)
    step = min(cap, 256)

    def build(h, dst):
        for k in range(0, cap, step):
            ids = lax.broadcasted_iota(jnp.int32, (step, elements), 0) + (h * cap + k)
            hot = jnp.where(ids == target, 1.0, 0.0).astype(BF16)
            out = lax.dot_general(both, hot, (((1,), (1,)), ((), ())), preferred_element_type=F32)
            dst[:, k : k + step] = out[:ROWS] + out[ROWS:]

    def goal(i):
        top = groups - 1 - i
        return top - jnp.where(top <= g, 1, 0)

    def bucket_copy(i, rows):
        return pltpu.make_async_remote_copy(
            src_ref=bsend.at[i, pl.ds(0, rows)],
            dst_ref=bucket.at[g, pl.ds(0, rows)],
            send_sem=bsend_sem.at[i],
            recv_sem=brecv_sem.at[g],
            device_id=(goal(i), p),
            device_id_type=MESH,
        )

    main = ROWS - SHARE

    def hop_in():
        return pltpu.make_async_remote_copy(
            src_ref=bsend.at[0, pl.ds(main, SHARE)], dst_ref=brelay, send_sem=hop_sem.at[0], recv_sem=hop_sem.at[1],
            device_id=(2, p), device_id_type=MESH,
        )

    def hop_out():
        return pltpu.make_async_remote_copy(
            src_ref=brelay, dst_ref=bucket.at[0, pl.ds(main, SHARE)], send_sem=hop_sem.at[2], recv_sem=hop_sem.at[3],
            device_id=(3, p), device_id_type=MESH,
        )

    def for_goal(i, act):
        for h in (groups - 1 - i, groups - 2 - i):
            hit = goal(i) == h
            if i == 0 and h == groups - 1:
                @pl.when(g == 0)
                def _():
                    act(hop_in())
                    act(bucket_copy(0, main))

                hit = jnp.logical_and(hit, g != 0)

            @pl.when(hit)
            def _(h=h):
                act(bucket_copy(i, SENT[h]))

    build(goal(0), bsend.at[0])
    pl.semaphore_wait(barrier, 3 * groups - 1)
    for i in range(1, groups - 1):
        build(goal(i), bsend.at[i])
        for_goal(i - 1, lambda copy: copy.start())
    build(g, bucket.at[g])
    for_goal(groups - 2, lambda copy: copy.start())

    for load in loads[6:]:
        load.wait()

    own_nodes = (g + 2) * (g + 3) * (g + 4) // 6
    wide[0, 0:NPM, 0 : FPTS * FACES] = tmat_ref[:, 0, :]
    wide[1, 0:NPM, 0 : FPTS * FACES] = lmat_ref[:, 0, :]
    wide[2, 0:NPM, 0 : 3 * NPM] = dmat_ref[:, 0, :]
    i, r = iotas((FACES * PP, LANES))
    order_points = ones_where((r == (i & (PP - 1)) * FACES + (i // PP)) & ((i & (PP - 1)) < FPTS))
    trace = exact_dot(order_points, wide[0], ((1,), (1,)))
    lift = exact_dot(wide[1, 0:DP], order_points, ((1,), (1,)))
    row = lax.broadcasted_iota(jnp.int32, (DP, FACES * PP), 0)
    lift = jnp.where(row < own_nodes, lift, 0.0)

    def weight_copy(kind, h):
        src, dst, send, recv = (
            (lift_out, lift_in, l_send, l_recv.at[0]),
            (trace_out, trace_in.at[0], t_send, t_recv.at[0]),
            (trace_out, trace_in.at[1], t_send, t_recv.at[1]),
        )[kind]
        return pltpu.make_async_remote_copy(
            src_ref=src, dst_ref=dst, send_sem=send.at[h], recv_sem=recv, device_id=(h, p), device_id_type=MESH
        )

    trace_out[...] = trace
    lift_out[...] = jnp.zeros((8, LANES), F32)
    lift_out[:, 0 : FACES * PP] = lift[0:8]

    tr_f = [[] for _ in range(FACES)]
    node = lax.broadcasted_iota(jnp.int32, (NPM, ROWS), 0)
    for at in range(0, 3 * COMPS * DP, DP):
        dx_h[at + DP - 8 : at + DP, :] = jnp.zeros((8, ROWS), BF16)
        dx_l[at + DP - 8 : at + DP, :] = jnp.zeros((8, ROWS), BF16)
    for c in range(COMPS):
        i, r, at = place(c, (LANES, ROWS))
        spread = ones_where((r == at) & (i < own_nodes) & (i < NPM))
        part = exact_dot(trace, spread)
        for f in range(FACES):
            tr_f[f].append(part[f * PP : (f + 1) * PP])
        block = exact_dot(wide[2], spread, ((0,), (0,)))
        for a in range(3):
            piece = split(jnp.where(node < own_nodes, block[a * NPM : (a + 1) * NPM], 0.0))
            at_row = (a * COMPS + c) * DP
            dx_h[at_row : at_row + NPM, :] = piece[0]
            dx_l[at_row : at_row + NPM, :] = piece[1]
    tr_f = [jnp.concatenate(parts + [jnp.zeros((LANES - TR, ROWS), F32)], 0) for parts in tr_f]

    def face_copy(s, j):
        return pltpu.make_async_remote_copy(
            src_ref=faces_out.at[j * groups + s],
            dst_ref=faces_in.at[j],
            send_sem=fsend_sem.at[j * groups + s],
            recv_sem=frecv_sem.at[j],
            device_id=(s, lax.rem(p - j + 1 + doms, doms)),
            device_id_type=MESH,
        )

    def face_local():
        return pltpu.make_async_copy(faces_out.at[groups], faces_in.at[1], frecv_sem.at[1])

    @pl.when(g == 0)
    def _():
        lift_in[...] = lift_out[...]
        for kind in range(2):
            for h in range(1, groups):
                weight_copy(kind, h).start()
        rows = slots // LANES
        count = -(-(3 * groups * blocks) // 8) * 8
        found = jnp.zeros((count, LANES), F32)
        per = recv_ref.shape[1]
        for f in range(1, FACES):
            entry = jnp.concatenate(
                [flat_row(recv_ref[k]) for k in range(f * rows // per, (f + 1) * rows // per)], axis=1
            )
            upper, lower = entry // LANES, entry & (LANES - 1)
            a = jnp.where(lax.broadcasted_iota(jnp.int32, (count, slots), 0) == upper, float(f), 0.0).astype(BF16)
            b = jnp.where(lax.broadcasted_iota(jnp.int32, (LANES, slots), 0) == lower, 1.0, 0.0).astype(BF16)
            found = found + lax.dot_general(a, b, (((1,), (1,)), ((), ())), preferred_element_type=F32)
        for n in range(3 * groups):
            faces_out[n, 0:blocks, :] = found[n * blocks : (n + 1) * blocks]
        for s in range(groups):
            for j in range(3):
                (face_local() if (s, j) == (0, 1) else face_copy(s, j)).start()

    @pl.when(g == 1)
    def _():
        trace_in[1] = trace_out[...]
        for h in range(2, groups):
            weight_copy(2, h).start()

    @pl.when(g != 0)
    def _():
        weight_copy(0, 1).wait_recv()

    i, r = iotas((LOW, 8))
    picked = exact_dot(ones_where(r == (i & (N1 - 1))), lift_in[...])
    for f in range(FACES):
        i, r = iotas((LANES, LANES))
        fan = ones_where(i == f * PP + (r & (PP - 1)))
        i, r = iotas((LOW, LANES))
        l1x[f * LOW : (f + 1) * LOW, :] = jnp.where((r // PP) == (i // N1), exact_dot(picked, fan), 0.0)

    for f in range(FACES):
        at = f * 2 * LANES
        for k, piece in enumerate(split(tr_f[f])):
            (tr_h, tr_l)[k][f * TR : (f + 1) * TR, :] = piece[:TR]
            (wcat_h, wcat_l)[k][at : at + LANES, :] = piece
        lowered = exact_dot(l1x[...], tr_f[f])
        filled = jnp.concatenate([lowered, jnp.zeros((LANES - TR, ROWS), F32)], 0)
        for k, piece in enumerate(split(filled)):
            (wcat_h, wcat_l)[k][at + LANES : at + 2 * LANES, :] = piece

        @pl.when(g < 2)
        def _(f=f, at=at):
            used = COMPS * own_nodes
            i, r = iotas((LANES, ROWS))
            coded = jnp.where((i < used) & (r == GEO + i), 1.0, 0.0) + jnp.where((i == used) & (r == ONE), float(f), 0.0)
            wcat_h[at : at + LANES, :] = coded.astype(BF16)
            wcat_l[at : at + LANES, :] = jnp.zeros((LANES, ROWS), BF16)

        @pl.when(g == 0)
        def _(f=f, lowered=lowered):
            i, r = iotas((TR, TR))
            pick = ones_where(((i & (PP - 1)) < N1) & (r == f * LOW + (i // PP) * N1 + (i & (PP - 1))))
            for k, piece in enumerate(split(exact_dot(pick, lowered))):
                (tr_h, tr_l)[k][f * TR : (f + 1) * TR, :] = piece

    i, r = iotas((DP, FACES * PP))
    unit = ones_where((i < N1) & ((r & (PP - 1)) == i))
    lift_ref[...] = jnp.zeros_like(lift_ref)
    for c in range(TOGETHER):
        lift_ref[c * DP : (c + 1) * DP, c * FACES * PP : (c + 1) * FACES * PP] = jnp.where(g == 0, unit, lift)

    for t in (table, low_table):
        t[FACES * slots : FACES * slots + 8, :] = jnp.zeros((8, LANES), F32)

    def make_tables(b):
        coefs = split(bucket[b].T)
        for f in range(FACES):
            w = tuple(x[f * 2 * LANES : (f + 1) * 2 * LANES, :] for x in (wcat_h, wcat_l))
            rows = dot3(coefs, w, ((1,), (1,)))
            at = pl.multiple_of(f * slots + b * cap, LANES)
            table[pl.ds(at, cap), :] = rows[:, :LANES]
            low_table[pl.ds(at, cap), :] = rows[:, LANES:]

    def arrival(b, rows):
        return pltpu.make_async_remote_copy(
            src_ref=bsend.at[0, pl.ds(0, rows)], dst_ref=bucket.at[b, pl.ds(0, rows)], send_sem=bsend_sem.at[0],
            recv_sem=brecv_sem.at[b], device_id=(b, p), device_id_type=MESH,
        )

    def arrive(b):
        for h in range(groups):
            hit = g == h
            if h == groups - 1:
                @pl.when(jnp.logical_and(hit, b == 0))
                def _():
                    arrival(b, main).wait_recv()
                    hop_out().wait_recv()

                hit = jnp.logical_and(hit, b != 0)

            @pl.when(hit)
            def _(h=h):
                arrival(b, SENT[h]).wait_recv()

    @pl.when(g == 2)
    def _():
        hop_in().wait_recv()
        hop_out().start()

    def table_step(k, _):
        b = lax.rem(g - k + groups, groups)

        @pl.when(k > 0)
        def _():
            arrive(b)

        make_tables(b)
        return 0

    lax.fori_loop(0, groups, table_step, 0)

    def list_copy(j, h, rows):
        n = j * groups + h
        return pltpu.make_async_remote_copy(
            src_ref=sbuf.at[n, pl.ds(0, rows)], dst_ref=arrived.at[j * groups + g, pl.ds(0, rows)], send_sem=ssem.at[n],
            recv_sem=rsem.at[j * groups + g], device_id=(h, dom_of(j)), device_id_type=MESH,
        )

    def local_copy(h, rows):
        n = groups + h
        return pltpu.make_async_copy(sbuf.at[n, pl.ds(0, rows)], arrived.at[n, pl.ds(0, rows)], rsem.at[n])

    def relay_in(k):
        j = RELAYED[k]
        n = j * groups + 1
        return pltpu.make_async_remote_copy(
            src_ref=sbuf.at[n], dst_ref=relay.at[k], send_sem=ssem.at[n], recv_sem=relay_recv.at[k],
            device_id=(0, dom_of(j)), device_id_type=MESH,
        )

    def relay_out(k):
        j = RELAYED[k]
        return pltpu.make_async_remote_copy(
            src_ref=relay.at[k], dst_ref=arrived.at[j * groups + 2], send_sem=relay_send.at[k],
            recv_sem=rsem.at[j * groups + 2], device_id=(1, p), device_id_type=MESH,
        )

    def width_cases():
        return ((g == 0, CODED[0]), (g == 1, CODED[1]), (g >= 2, TR))

    def for_list(j, h, act, act_local):
        here = jnp.logical_and(j == 1, h == g)
        hop = jnp.logical_and(jnp.logical_and(g == 2, h == 1), j != 1)
        plain = jnp.logical_not(jnp.logical_or(here, hop))
        for hit, rows in width_cases():
            @pl.when(jnp.logical_and(hit, plain))
            def _(rows=rows):
                act(list_copy(j, h, rows))

            @pl.when(jnp.logical_and(hit, here))
            def _(rows=rows):
                act_local(local_copy(h, rows))
        for k in range(len(RELAYED)):
            @pl.when(jnp.logical_and(hop, j == RELAYED[k]))
            def _(k=k):
                act(relay_in(k))

    def for_low(j, act, act_local):
        here = jnp.logical_and(j == 1, g == 0)

        @pl.when(jnp.logical_not(here))
        def _():
            act(list_copy(j, 0, LOW))

        @pl.when(here)
        def _():
            act_local(local_copy(0, LOW))

    def turn(k):
        return jnp.where(k == 0, 2, k - 1)

    def which(k):
        pos, lap = lax.rem(k, 3), k // 3
        first = jnp.where(g == 1, 1, jnp.where(g == 2, 1, 2))
        second = jnp.where(g == 1, 2, jnp.where(g == 2, 3, 1))
        third = jnp.where(g == 2, 2, 3)
        j = jnp.where(lap == 2, 1, jnp.where(lax.rem(lap + pos, 2) == 0, 2, 0))
        return j, jnp.where(pos == 0, first, jnp.where(pos == 1, second, third))

    def start(copy):
        copy.start()

    many = 3 * (groups - 1)

    def one_list(k, _):
        j, h = which(k)
        n = j * groups + h
        for q in range(blocks):
            gather_block(send_ref.at[n * pairs + q // 2], q % 2, table, tmp.at[q % 2])
            sbuf[n, :, q * LANES : (q + 1) * LANES] = tmp[q % 2].T[:TR]
            if q == 1:
                @pl.when(k > 0)
                def _():
                    for_list(*which(k - 1), start, start)
        return 0

    lax.fori_loop(0, many, one_list, 0)

    def low_list(k, _):
        j = turn(k)
        n = j * groups

        @pl.when(jnp.logical_or(g != 0, j != 1))
        def _():
            pltpu.make_async_remote_copy(
                src_ref=faces_out.at[0], dst_ref=faces_in.at[j], send_sem=fsend_sem.at[0],
                recv_sem=frecv_sem.at[j], device_id=(0, dom_of(j)), device_id_type=MESH,
            ).wait_recv()

        @pl.when(jnp.logical_and(g == 0, j == 1))
        def _():
            face_local().wait()

        for q in range(blocks):
            gather_block(send_ref.at[n * pairs + q // 2], q % 2, low_table, tmp.at[q % 2])
            block = tmp[q % 2].T[:TR]
            face = faces_in[j, q : q + 1, :]
            sbuf[n, 0:LOW, q * LANES : (q + 1) * LANES] = functools.reduce(
                lambda x, y: x + y,
                [jnp.where(face == float(f), block[f * LOW : (f + 1) * LOW], 0.0) for f in range(FACES)],
            )
            if q == 1:
                @pl.when(k == 0)
                def _():
                    for_list(*which(many - 1), start, start)

                @pl.when(k > 0)
                def _():
                    for_low(turn(k - 1), start, start)
        return 0

    lax.fori_loop(0, 3, low_list, 0)
    for_low(turn(2), start, start)

    def volume_step(b, _):
        block = bucket.at[b]
        pieces = split(block[...])
        geo_ref[b] = block[0:GROWS, :]
        derivs[...] = dot3((dx_h[...], dx_l[...]), pieces, ((1,), (0,)))
        for c in range(COMPS):
            q1, x1, q2, x2 = CURL[c]
            total = None
            for a in range(3):
                for q, x, sign in ((q1, x1, 1), (q2, x2, -1)):
                    m = block[METRIC + 3 * a + x : METRIC + 3 * a + x + 1, :]
                    at = (a * COMPS + q) * DP
                    term = m * derivs[at : at + DP, :]
                    total = term if total is None else (total + term if sign > 0 else total - term)
            vol_ref[b, c * DP : (c + 1) * DP, :] = total
        for f in range(FACES):
            w = tuple(x[f * TR : (f + 1) * TR, :] for x in (tr_h, tr_l))
            own_ref[b, f] = dot3(w, pieces, ((1,), (0,)))
        return 0

    lax.fori_loop(0, groups, volume_step, 0)

    @pl.when(g != 0)
    def _():
        weight_copy(1, 1).wait_recv()

        @pl.when(g > 1)
        def _():
            weight_copy(2, 2).wait_recv()

        for s in range(2):
            for f in range(FACES):
                i, r = iotas((TR, FACES * PP))
                fan = ones_where(r == f * PP + (i & (PP - 1)))
                _, at_node, _ = coded_rows(s, (CODED[s], LANES), 0)
                _, r = iotas((CODED[s], LANES))
                rows = exact_dot(exact_dot(fan, trace_in[s]), ones_where(r == at_node), ((1,), (1,)))
                comp, _, valid = coded_rows(s, (TR, CODED[s]), 1)
                i, _ = iotas((TR, CODED[s]))
                pieces = split(jnp.where(((i // PP) == comp) & valid, rows, 0.0))
                tx_h[s, f * TR : (f + 1) * TR, 0 : CODED[s]] = pieces[0]
                tx_l[s, f * TR : (f + 1) * TR, 0 : CODED[s]] = pieces[1]

    @pl.when(g == 0)
    def _():
        for k in range(len(RELAYED)):
            relay_in(k).wait_recv()
            relay_out(k).start()

    lists = 3 * groups
    far_ref[lists * list_size : lists * list_size + 8, :] = jnp.zeros((8, LANES), F32)
    fill = jnp.zeros((LANES - TR, LANES), F32)

    def got(l, j, s, rows):
        return pltpu.make_async_remote_copy(
            src_ref=sbuf.at[l, pl.ds(0, rows)], dst_ref=arrived.at[l, pl.ds(0, rows)], send_sem=ssem.at[l],
            recv_sem=rsem.at[l], device_id=(s, dom_of(j)), device_id_type=MESH,
        )

    def take(k, _):
        j = turn(k)
        for s in range(groups):
            l = j * groups + s
            rows = CODED[s] if s < 2 else TR
            here = jnp.logical_and(j == 1, g == s)
            away = jnp.logical_not(here)
            for hit, size in ((g == 0, LOW), (g != 0, rows)):
                @pl.when(jnp.logical_and(hit, away))
                def _(size=size, l=l, s=s):
                    got(l, j, s, size).wait_recv()

            @pl.when(here)
            def _(s=s, rows=rows):
                local_copy(s, rows if s else LOW).wait()

            def put(q, block, l=l):
                at = pl.multiple_of(l * list_size + q * LANES, LANES)
                far_ref[pl.ds(at, LANES), :] = jnp.concatenate([block, fill], 0).T

            @pl.when(g == 0)
            def _(l=l, put=put):
                gap = jnp.zeros((PP - N1, LANES), F32)
                for q in range(blocks):
                    x = arrived[l, 0:LOW, q * LANES : (q + 1) * LANES]
                    parts = []
                    for c in range(COMPS):
                        parts += [x[c * N1 : (c + 1) * N1], gap]
                    put(q, jnp.concatenate(parts, 0))

            @pl.when(g != 0)
            def _(l=l, s=s, put=put, rows=rows):
                if s > 1:
                    for q in range(blocks):
                        put(q, arrived[l, :, q * LANES : (q + 1) * LANES])
                    return
                used = COMPS * NODES[s]
                w = (tx_h[s, :, 0:rows], tx_l[s, :, 0:rows])
                for q in range(0, blocks, 2):
                    x = arrived[l, 0:rows, q * LANES : (q + 2) * LANES]
                    spread = dot3(w, split(x), ((1,), (0,)))
                    face = x[used : used + 1, :]
                    block = functools.reduce(
                        lambda u, v: u + v,
                        [jnp.where(face == float(f), spread[f * TR : (f + 1) * TR], 0.0) for f in range(FACES)],
                    )
                    put(q, block[:, :LANES])
                    put(q + 1, block[:, LANES:])
        return 0

    lax.fori_loop(0, 3, take, 0)

    def sent(copy):
        copy.wait_send()

    def nothing(copy):
        pass

    for i in range(groups - 1):
        for_goal(i, sent)

    def list_sent(k, _):
        j, h = which(k)
        here = jnp.logical_and(j == 1, h == g)
        for hit, rows in width_cases():
            @pl.when(jnp.logical_and(hit, jnp.logical_not(here)))
            def _(rows=rows):
                list_copy(j, h, rows).wait_send()
        return 0

    def low_sent(k, _):
        j = turn(k)

        @pl.when(jnp.logical_or(g != 0, j != 1))
        def _():
            list_copy(j, 0, LOW).wait_send()

        return 0

    lax.fori_loop(0, many, list_sent, 0)
    lax.fori_loop(0, 3, low_sent, 0)

    @pl.when(g == 2)
    def _():
        hop_out().wait_send()

    @pl.when(g == 1)
    def _():
        for h in range(2, groups):
            weight_copy(2, h).wait_send()

    @pl.when(g == 0)
    def _():
        for k in range(len(RELAYED)):
            relay_out(k).wait_send()
        for kind in range(2):
            for h in range(1, groups):
                weight_copy(kind, h).wait_send()
        for s in range(groups):
            for j in range(3):
                if (s, j) != (0, 1):
                    face_copy(s, j).wait_send()


def cross_of(u, v):
    return [u[1] * v[2] - u[2] * v[1], u[2] * v[0] - u[0] * v[2], u[0] * v[1] - u[1] * v[0]]


def final_kernel(
    groups, cap, recv_ref, table, own_ref, vol_ref, geo_ref, lift_ref, out_hbm,
    tmp, far, flux, out, index, index_sem, out_sem,
):
    slots = groups * cap
    blocks = cap // LANES
    lift = split(lift_ref[...])

    def fetch(g, f):
        return pltpu.make_async_copy(recv_ref.at[f * groups + g], index.at[f], index_sem.at[f])

    def leave(g):
        return pltpu.make_async_copy(out.at[g % 2], out_hbm.at[:, pl.ds(g * cap, cap)], out_sem.at[g % 2])

    for f in range(FACES):
        fetch(0, f).start()

    def gather_face(g, f):
        fetch(g, f).wait()
        for q in range(blocks):
            gather_block(index.at[f], q, table, tmp.at[q % 2])
            far[g % 2, f, :, q * LANES : (q + 1) * LANES] = tmp[q % 2].T[:TR]
        if g < groups - 1:
            fetch(g + 1, f).start()

    def flux_face(g, f):
        jump = far[g % 2, f] - own_ref[g, f]
        jumps = [jump[c * PP : (c + 1) * PP, :] for c in range(COMPS)]
        n = [geo_ref[g, NORMAL + c * FACES + f : NORMAL + c * FACES + f + 1, :] for c in range(3)]
        s = 0.5 * geo_ref[g, SCALE + f : SCALE + f + 1, :]
        je, jh = jumps[:3], jumps[3:]
        ne = n[0] * je[0] + n[1] * je[1] + n[2] * je[2]
        nh = n[0] * jh[0] + n[1] * jh[1] + n[2] * jh[2]
        th, te = cross_of(n, jh), cross_of(n, je)
        for c in range(3):
            at = (c * FACES + f) * PP
            flux[at : at + PP, :] = s * (th[c] + je[c] - n[c] * ne)
            at += 3 * FACES * PP
            flux[at : at + PP, :] = s * (jh[c] - te[c] - n[c] * nh)

    for f in range(FACES):
        gather_face(0, f)
    for g in range(groups):
        for f in range(FACES):
            if g < groups - 1:
                gather_face(g + 1, f)
            flux_face(g, f)
        if g > 1:
            leave(g - 2).wait()
        for c in range(0, COMPS, TOGETHER):
            count = min(TOGETHER, COMPS - c)
            deep = count * FACES * PP
            w = tuple(x[: count * DP, :deep] for x in lift)
            lifted = dot3(w, split(flux[c * FACES * PP : c * FACES * PP + deep, :]), ((1,), (0,)))
            lifted = lifted + vol_ref[g, c * DP : (c + count) * DP, :]
            for k in range(count):
                out[g % 2, (c + k) * NPM : (c + k + 1) * NPM, :] = lifted[k * DP : k * DP + NPM]
        leave(g).start()
    leave(groups - 2).wait()
    leave(groups - 1).wait()


def local(groups, doms, fields, metric, normals, fscale, orders, slots, send_faces, recv_faces, dmat, tmat, lmat):
    elements = fields.shape[1]
    cap = elements // 2
    total = groups * cap
    lists = 3 * groups
    list_size = send_faces.shape[0] // lists
    blocks = list_size // LANES
    dma = pltpu.SemaphoreType.DMA
    i32 = jnp.int32
    vmem = pltpu.VMEM
    recv_shape = (FACES * groups, cap // LANES, LANES)
    received, own, vol, geo, lift, entries = pl.pallas_call(
        functools.partial(move_kernel, groups, doms, cap, list_size),
        out_shape=(
            jax.ShapeDtypeStruct((lists * list_size + 8, LANES), F32),
            jax.ShapeDtypeStruct((groups, FACES, TR, cap), F32),
            jax.ShapeDtypeStruct((groups, COMPS * DP, cap), F32),
            jax.ShapeDtypeStruct((groups, GROWS, cap), F32),
            jax.ShapeDtypeStruct((TOGETHER * DP, TOGETHER * FACES * PP), F32),
            jax.ShapeDtypeStruct(recv_shape, i32),
        ),
        in_specs=[HB] * 11,
        out_specs=(VM,) * 6,
        scratch_shapes=[
            vmem((elements // LANES, LANES), i32),
            vmem((elements // LANES, LANES), i32),
            vmem(fields.shape, F32),
            vmem(metric.shape, F32),
            vmem(normals.shape, F32),
            vmem(fscale.shape, F32),
            vmem((NPM, 1, 3 * NPM), F32),
            vmem((NPM, 1, FPTS * FACES), F32),
            vmem((NPM, 1, FPTS * FACES), F32),
            pltpu.SMEM((lists * blocks // 2, 2, LANES), i32),
            dma((11,)),
            vmem((ROWS, elements), F32),
            vmem((groups - 1, ROWS, cap), F32),
            vmem((groups, ROWS, cap), F32),
            vmem((SHARE, cap), F32),
            vmem((FACES * total + 8, LANES), F32),
            vmem((FACES * total + 8, LANES), F32),
            vmem((2, LANES, LANES), F32),
            vmem((lists, TR, list_size), F32),
            vmem((lists, TR, list_size), F32),
            vmem((len(RELAYED), TR, list_size), F32),
            vmem((3, LANES, LANES), F32),
            vmem((2 * FACES * LANES, ROWS), BF16),
            vmem((2 * FACES * LANES, ROWS), BF16),
            vmem((FACES * TR, ROWS), BF16),
            vmem((FACES * TR, ROWS), BF16),
            vmem((3 * COMPS * DP, ROWS), BF16),
            vmem((3 * COMPS * DP, ROWS), BF16),
            vmem((2, FACES * TR, LANES), BF16),
            vmem((2, FACES * TR, LANES), BF16),
            vmem((3 * COMPS * DP, cap), F32),
            vmem((FACES * LOW, LANES), F32),
            vmem((8, LANES), F32),
            vmem((8, LANES), F32),
            vmem((FACES * PP, LANES), F32),
            vmem((2, FACES * PP, LANES), F32),
            vmem((lists, 8, LANES), F32),
            vmem((3, 8, LANES), F32),
            dma((groups - 1,)),
            dma((groups,)),
            dma((4,)),
            dma((lists,)),
            dma((lists,)),
            dma((len(RELAYED),)),
            dma((len(RELAYED),)),
            dma((groups,)),
            dma((1,)),
            dma((groups,)),
            dma((2,)),
            dma((lists,)),
            dma((3,)),
        ],
        compiler_params=pltpu.CompilerParams(
            vmem_limit_bytes=40 * 1024 * 1024, collective_id=0, has_side_effects=True
        ),
        name="move",
    )(
        *[
            pltpu.with_memory_space_constraint(x, pltpu.HBM)
            for x in (
                send_faces.reshape(-1, 2, LANES),
                orders.reshape(-1, LANES),
                slots.reshape(-1, LANES),
                fields,
                metric,
                normals,
                fscale,
                recv_faces.reshape(recv_shape),
                jnp.transpose(dmat, (2, 0, 1)),
                jnp.transpose(tmat, (2, 0, 1)),
                jnp.transpose(lmat, (1, 0, 2)),
            )
        ]
    )
    return pl.pallas_call(
        functools.partial(final_kernel, groups, cap),
        out_shape=jax.ShapeDtypeStruct((COMPS * NPM, total), F32),
        in_specs=[VM] * 6,
        out_specs=HB,
        scratch_shapes=[
            vmem((2, LANES, LANES), F32),
            vmem((2, FACES, TR, cap), F32),
            vmem((COMPS * FACES * PP, cap), F32),
            vmem((2, COMPS * NPM, cap), F32),
            pltpu.SMEM((FACES, cap // LANES, LANES), i32),
            dma((FACES,)),
            dma((2,)),
        ],
        compiler_params=pltpu.CompilerParams(vmem_limit_bytes=24 * 1024 * 1024),
        name="final",
    )(entries, received, own, vol, geo, lift)


def solution(mesh):
    col = P(None, ("grp", "dom"))
    row = P(("grp", "dom"))
    mat = P("grp", None, None)
    in_specs = (col, col, col, col, row, row, row, row, mat, mat, mat)
    body = functools.partial(local, mesh.shape["grp"], mesh.shape["dom"])
    return jax.shard_map(body, mesh=mesh, in_specs=in_specs, out_specs=col, check_vma=False)
```
